32 devices in a mesh: seq: 8 (over z, x), head: 2 (over y), dp: 2 (over core).
Axes of the slice: x: 2, y: 2, z: 4, core: 2. Of those that a mesh axis runs over, the one named last changes fastest.
Arguments:
- queries: bfloat16 [8192, 4096], P(('dp', 'seq'), 'head'), parts along dimension 0, may hold values from -200 to 200
- keys: bfloat16 [8192, 1024], P(('dp', 'seq'), 'head'), parts along dimension 0, may hold values from -4 to 4
- values: bfloat16 [8192, 1024], P(('dp', 'seq'), 'head'), parts along dimension 0, may hold values from -15 to 15
- doc_ids: int32 [8192], P(('dp', 'seq')), parts along dimension 0, may hold values from 0 to 7, as said below
- block_lists: int32 [64, 16], P(('dp', 'seq')), parts along dimension 0, may hold values from 0 to 32, as said below
- w_out: bfloat16 [4096, 4096], P('head'), may hold values from -0.09375 to 0.09375
Outputs:
- mixed: bfloat16 [8192, 4096], P(('dp', 'seq'), 'head'), parts along dimension 0
The draws below stay inside these ranges and needn't reach their ends.
There are 2 independent parts, one for each index of `dp`. The reference program is written for one: setup_inputs(seed, part) draws one part's arguments, and reference() takes and returns one part's arrays. A program takes and returns all parts, laid end to end along the dimension named above; an argument that names none is the same for every part. Nothing has to cross between parts.
Inputs may be any that keep to these rules, and one draw needn't show every extreme that they name: `block_lists`: row i lists the blocks that query block i reads: 16 entries, each a block of the sequence or the null value 32; the non-null entries of a row are distinct and include i. Blocks k * 4 to k * 4 + 3 lie on index k of seq; over the rows of one index of seq together, at most one distinct block of each other index of seq is named (so each index of seq sends at most one of its blocks to each other index). `doc_ids`: never falling along the sequence.
All inputs are finite; a program needn't handle non-finite values.
Results may differ from the reference program's by a relative error of at most 0.013.
Values may be sent and summed in bfloat16 or wider, within the bound.
A program may use at most 128 MiB of HBM per device.

```python
import math
import jax
import jax.numpy as jnp
from jax import lax

D = 4096
QUERY_HEADS = 32
KEY_VALUE_HEADS = 8
HEAD_SIZE = 128
BLOCK_TOKENS = 128
TOPK = 16
DOCS = 8
SEQUENCE_TOKENS = 4096
BPD = 4
BLOCK_TOTAL = 32
N_HEAD = 2


def draw_queries(key, part):
    base_index = 2.0 * jax.random.truncated_normal(jax.random.fold_in(key, 21), -4.0, 4.0, (SEQUENCE_TOKENS, QUERY_HEADS * HEAD_SIZE), jnp.float32)
    return base_index.astype(jnp.bfloat16)


def draw_keys(key, part):
    base_index = jax.random.truncated_normal(jax.random.fold_in(key, 22), -4.0, 4.0, (SEQUENCE_TOKENS, KEY_VALUE_HEADS * HEAD_SIZE), jnp.float32)
    return base_index.astype(jnp.bfloat16)


def draw_doc_ids(key, part):
    first_len = jax.random.randint(jax.random.fold_in(key, 41), (1,), SEQUENCE_TOKENS * 5 // 8, SEQUENCE_TOKENS * 3 // 4, dtype=jnp.int32)
    others = jax.random.randint(jax.random.fold_in(key, 42), (DOCS - 2,), 0, SEQUENCE_TOKENS, dtype=jnp.int32)
    others = first_len + 1 + others % (SEQUENCE_TOKENS - first_len - 1)
    bounds = jnp.concatenate([first_len, others]).astype(jnp.int32)
    positions = jnp.arange(SEQUENCE_TOKENS, dtype=jnp.int32)
    return jnp.sum((positions[:, None] >= bounds[None, :]).astype(jnp.int32), axis=1).astype(jnp.int32)


def draw_block_lists(key, part):
    seq_devices = BLOCK_TOTAL // BPD
    remote = min(TOPK - BPD, seq_devices - 1)
    padding = TOPK - BPD - remote
    offsets = jax.random.randint(jax.random.fold_in(key, 31), (seq_devices, seq_devices), 0, BPD, dtype=jnp.int32)
    owner_ids = jnp.arange(seq_devices, dtype=jnp.int32)

    def one_row(row):
        device = row // BPD
        shuffled = jax.random.permutation(jax.random.fold_in(jax.random.fold_in(key, 32), row), seq_devices).astype(jnp.int32)
        distance = jnp.abs(owner_ids - device)
        score = shuffled + 1 + jnp.where(distance <= 2, 4 * seq_devices, 0)
        score = score + jnp.where(owner_ids == (device + seq_devices // 2) % seq_devices, 2 * seq_devices, 0)
        score = jnp.where(owner_ids != device, score, 0)
        best, chosen = lax.top_k(score, remote)
        picked = jnp.where(best > 0, chosen * BPD + offsets[device, chosen], BLOCK_TOTAL).astype(jnp.int32)
        own_blocks = (device * BPD + jnp.arange(BPD, dtype=jnp.int32)).astype(jnp.int32)
        return jnp.concatenate([own_blocks, picked, jnp.full((padding,), BLOCK_TOTAL, jnp.int32)])
    return jax.vmap(one_row)(jnp.arange(BLOCK_TOTAL, dtype=jnp.int32))


def block_scale(key, shape, cuts, smallest, high):
    factor_of, own = 1.0, jax.random.fold_in(key, 6)
    for position, parts in cuts:
        heights = jnp.exp(jax.random.uniform(jax.random.fold_in(own, position), (parts,), jnp.float32, smallest / len(cuts), high / len(cuts)))
        factor_of = factor_of * jnp.repeat(heights, shape[position] // parts).reshape([-1 if axis == position else 1 for axis in range(len(shape))])
    return factor_of


def bell_draw(own_key, extent, scale, reach, shards=(), kind=jnp.bfloat16):
    array = scale * jax.random.normal(own_key, extent, jnp.float32)
    if shards:
        array = array * block_scale(own_key, extent, shards, -0.22, 0.18)
    return jnp.clip(array, -reach, reach).astype(kind)


def setup_inputs(seed: int = 0, part: int = 0) -> dict:
    splits = jax.random.split(jax.random.key(seed), 7)
    part_splits = jax.random.split(jax.random.fold_in(splits[6], part), 7)
    queries = draw_queries(jax.random.fold_in(jax.random.fold_in(splits[6], part), 71), part)
    keys = draw_keys(jax.random.fold_in(jax.random.fold_in(splits[6], part), 71), part)
    values = bell_draw(part_splits[2], (SEQUENCE_TOKENS, KEY_VALUE_HEADS * HEAD_SIZE), 3.0, 15.0, ((0, 8), (1, 2)))
    doc_ids = draw_doc_ids(jax.random.fold_in(jax.random.fold_in(splits[6], part), 71), part)
    block_lists = draw_block_lists(jax.random.fold_in(jax.random.fold_in(splits[6], part), 71), part)
    w_out = bell_draw(splits[5], (QUERY_HEADS * HEAD_SIZE, D), (QUERY_HEADS * HEAD_SIZE) ** -0.5, 0.09375, ((0, 2),))
    return {"queries": queries, "keys": keys, "values": values, "doc_ids": doc_ids, "block_lists": block_lists, "w_out": w_out}


negative = -1e+30
far_position = 1073741824

def block_terms(query_block, key_rows, value_rows, allowed):
    scores = jnp.einsum('qhge,jkhe->hgqjk', query_block.astype(jnp.float32), key_rows.astype(jnp.float32)) * (1.0 / math.sqrt(HEAD_SIZE))
    masked = jnp.where(allowed[None, None], scores, negative)
    block_top = lax.optimization_barrier(jnp.max(masked, axis=-1))
    probs = jnp.where(allowed[None, None], jnp.exp(masked - block_top[..., None]), 0.0)
    block_sum = lax.optimization_barrier(jnp.sum(probs, axis=-1))
    weights = probs.astype(jnp.bfloat16)
    partial_value = jnp.einsum('hgqjk,jkhe->hgqje', weights.astype(jnp.float32), value_rows.astype(jnp.float32))
    return (block_top, block_sum, partial_value)

def finish(block_top, block_sum, partial_value):
    row_peak = lax.optimization_barrier(jnp.max(block_top, axis=-1))
    factor = jnp.exp(block_top - row_peak[..., None])
    numer = lax.optimization_barrier(jnp.sum(factor[..., None] * partial_value, axis=3))
    denom = lax.optimization_barrier(jnp.sum(factor * block_sum, axis=-1))
    result = numer / denom[..., None]
    rows = result.shape[2]
    return jnp.transpose(result, (2, 0, 1, 3)).reshape(rows, -1).astype(jnp.bfloat16)

def reference(queries, keys, values, doc_ids, block_lists, w_out):
    group_count = QUERY_HEADS // KEY_VALUE_HEADS
    positions = jnp.arange(SEQUENCE_TOKENS, dtype=jnp.int32)
    doc_range = jnp.arange(DOCS, dtype=jnp.int32)
    doc_match = doc_ids[:, None] == doc_range[None, :]
    firsts = lax.optimization_barrier(jnp.min(jnp.where(doc_match, positions[:, None], far_position), axis=0)).astype(jnp.int32)
    later = doc_range[None, :] > doc_range[:, None]
    ends_doc = lax.optimization_barrier(jnp.min(jnp.where(later, firsts[None, :], far_position), axis=1)).astype(jnp.int32)
    starts = lax.optimization_barrier(jnp.sum(jnp.where(doc_match, firsts[None, :], 0), axis=1)).astype(jnp.int32)
    ends = lax.optimization_barrier(jnp.sum(jnp.where(doc_match, ends_doc[None, :], 0), axis=1)).astype(jnp.int32)
    empty_block = jnp.zeros((1, BLOCK_TOKENS, KEY_VALUE_HEADS, HEAD_SIZE), jnp.bfloat16)
    key_lookup = jnp.concatenate([keys.reshape(BLOCK_TOTAL, BLOCK_TOKENS, KEY_VALUE_HEADS, HEAD_SIZE), empty_block], axis=0)
    value_lookup = jnp.concatenate([values.reshape(BLOCK_TOTAL, BLOCK_TOKENS, KEY_VALUE_HEADS, HEAD_SIZE), empty_block], axis=0)
    query_tiles = queries.reshape(BLOCK_TOTAL, BLOCK_TOKENS, KEY_VALUE_HEADS, group_count, HEAD_SIZE)
    inside = jnp.arange(BLOCK_TOKENS, dtype=jnp.int32)

    def per_block(inputs):
        query_block, lists_row, query_start, query_end = inputs
        key_rows = jnp.take(key_lookup, lists_row, axis=0)
        value_rows = jnp.take(value_lookup, lists_row, axis=0)
        usable = lists_row < BLOCK_TOTAL
        key_pos = lists_row[:, None] * BLOCK_TOKENS + inside[None, :]
        allowed = usable[None, :, None] & (key_pos[None] < query_end[:, None, None]) & (key_pos[None] >= query_start[:, None, None])
        return finish(*block_terms(query_block, key_rows, value_rows, allowed))
    attn = lax.map(per_block, (query_tiles, block_lists, starts.reshape(BLOCK_TOTAL, BLOCK_TOKENS), ends.reshape(BLOCK_TOTAL, BLOCK_TOKENS)))
    attn = attn.reshape(SEQUENCE_TOKENS, QUERY_HEADS * HEAD_SIZE)
    cols = QUERY_HEADS * HEAD_SIZE // N_HEAD

    def add_group(running, group):
        attn_cols = lax.dynamic_slice_in_dim(attn, group * cols, cols, 1)
        weight_rows = lax.dynamic_slice_in_dim(w_out, group * cols, cols, 0)
        part = jnp.dot(attn_cols, weight_rows, preferred_element_type=jnp.float32).astype(jnp.bfloat16)
        part = lax.optimization_barrier(part)
        return (running + part.astype(jnp.float32), None)
    summed, _ = lax.scan(add_group, jnp.zeros((SEQUENCE_TOKENS, D), jnp.float32), jnp.arange(N_HEAD, dtype=jnp.int32))
    return summed.astype(jnp.bfloat16)
```

```python
import functools
import math

import jax
import jax.numpy as jnp
from jax import lax
from jax.experimental import pallas as pl
from jax.experimental.pallas import tpu as pltpu
from jax.sharding import PartitionSpec as P

HEAD_SIZE = 128
BLOCK = 128
LANES = 128
DOCS = 8
GROUP = 4
PIECES = 2
TILE = 512
MESH = pl.DeviceIdType.MESH

far_score = float(2**20)
exp2_scale = math.log2(math.e) / math.sqrt(HEAD_SIZE)


def column_of(row):
    return jnp.broadcast_to(row, (BLOCK, LANES)).astype(jnp.float32).T


def kernel(
    seq_count,
    head_count,
    dp_count,
    lists_ref,
    docs_ref,
    q_hbm,
    k_hbm,
    v_hbm,
    w_hbm,
    out_hbm,
    q_ref,
    k_ref,
    v_ref,
    w_ref,
    note_out,
    note_in,
    stage,
    land,
    qext,
    kext,
    scores,
    probs,
    attn,
    ysend,
    yrecv,
    kept,
    done,
    load_sem,
    note_ssem,
    note_rsem,
    kv_ssem,
    kv_rsem,
    y_ssem,
    y_rsem,
    out_sem,
    turn_sem,
):
    own = lax.axis_index("seq")
    head = lax.axis_index("head")
    core = lax.axis_index("dp")
    blocks = docs_ref.shape[0]
    slots = blocks + seq_count - 1
    kv_heads = k_ref.shape[1] // HEAD_SIZE
    width = GROUP * HEAD_SIZE
    cols = kept.shape[1]
    piece = cols // PIECES
    tile = min(TILE, piece)
    others = head_count - 1

    loads = [
        pltpu.make_async_copy(src, dst, load_sem.at[n])
        for n, (src, dst) in enumerate(
            ((k_hbm, k_ref), (v_hbm, v_ref), (q_hbm, q_ref), (w_hbm, w_ref))
        )
    ]
    for load in loads:
        load.start()

    barrier = pltpu.get_barrier_semaphore()
    for d in range(1, seq_count):
        pl.semaphore_signal(
            barrier, inc=1, device_id={"seq": lax.rem(own + d, seq_count)}, device_id_type=MESH
        )
    for d in range(1, head_count):
        pl.semaphore_signal(
            barrier, inc=1, device_id={"head": lax.rem(head + d, head_count)}, device_id_type=MESH
        )
    for d in range(1, dp_count):
        pl.semaphore_signal(
            barrier, inc=1, device_id={"dp": lax.rem(core + d, dp_count)}, device_id_type=MESH
        )

    lane = lax.broadcasted_iota(jnp.int32, (1, LANES), 1)
    slot = lane - DOCS
    source = own - (slot - blocks + 1)
    source = jnp.where(source < 0, source + seq_count, source)
    is_own = (slot >= 0) & (slot < blocks)
    is_far = (slot >= blocks) & (slot < slots)
    low = jnp.where(is_own, own * blocks + slot, jnp.where(is_far, source * blocks, -1))
    high = jnp.where(is_own, low + 1, jnp.where(is_far, low + blocks, -1))
    owner_low = lane * blocks
    asked = jnp.zeros((1, LANES), jnp.int32)
    listed = []
    for i in range(blocks):
        here = jnp.zeros((1, LANES), jnp.int32)
        for j in range(lists_ref.shape[1]):
            block = lists_ref[i, j]
            here = jnp.where((block >= low) & (block < high), 1, here)
            inside = (block >= owner_low) & (block < owner_low + blocks)
            asked = jnp.maximum(asked, jnp.where(inside, block - owner_low + 1, 0))
        listed.append(here)
    note_out[0:blocks, :] = docs_ref[...]
    note_out[blocks : blocks + 1, :] = asked

    pl.semaphore_wait(barrier, seq_count + head_count + dp_count - 3)

    def note_copy(d):
        return pltpu.make_async_remote_copy(
            src_ref=note_out,
            dst_ref=note_in.at[d - 1],
            send_sem=note_ssem.at[d - 1],
            recv_sem=note_rsem.at[d - 1],
            device_id={"seq": lax.rem(own + d, seq_count)},
            device_id_type=MESH,
        )

    def kv_copy(d, h):
        return pltpu.make_async_remote_copy(
            src_ref=stage.at[d - 1, h],
            dst_ref=land.at[d - 1, h],
            send_sem=kv_ssem.at[d - 1, h],
            recv_sem=kv_rsem.at[d - 1, h],
            device_id={"seq": lax.rem(own + d, seq_count)},
            device_id_type=MESH,
        )

    def step_of(n):
        near = n // 2 + 1
        return jnp.where(lax.rem(n, 2) == 0, near, seq_count - near)

    for d in range(1, seq_count):
        note_copy(d).start()
    loads[0].wait()
    loads[1].wait()

    def fill(n, carry):
        d = step_of(n)
        note_copy(seq_count - d).wait_recv()
        row = note_in[seq_count - d - 1, blocks : blocks + 1, :]
        want = jnp.max(jnp.where(lane == own, row, 0), axis=1, keepdims=True)
        want = jnp.broadcast_to(jnp.maximum(want - 1, 0), (BLOCK, LANES))
        hots = [jnp.where(want == b, 1.0, 0.0).astype(jnp.bfloat16) for b in range(blocks)]
        for h in range(kv_heads):
            cut = slice(h * HEAD_SIZE, (h + 1) * HEAD_SIZE)
            for part, ref in enumerate((k_ref, v_ref)):
                picked = None
                for b in range(blocks):
                    term = ref[b * BLOCK : (b + 1) * BLOCK, cut] * hots[b]
                    picked = term if picked is None else picked + term
                stage[d - 1, h, part * BLOCK : (part + 1) * BLOCK, :] = picked
        return carry

    lax.fori_loop(0, seq_count - 1, fill, 0)

    @pl.when(core > 0)
    def _():
        pl.semaphore_wait(turn_sem, 1)

    def send_head(h, carry):
        def send(n, inner):
            kv_copy(step_of(n), h).start()
            return inner

        return lax.fori_loop(0, seq_count - 1, send, carry)

    lax.fori_loop(0, kv_heads, send_head, 0)

    lanes = lax.broadcasted_iota(jnp.int32, (BLOCK, LANES), 1)
    lanes_f = lanes.astype(jnp.float32)
    is_doc = lanes < DOCS

    def put_kext(s, row):
        same = jnp.where(column_of(row) == lanes_f, 1.0, 0.0)
        hot = jnp.where(is_doc, same, jnp.where(lanes == DOCS + s, 1.0, 0.0))
        at = s * BLOCK
        if not isinstance(s, int):
            at = pl.multiple_of(at, BLOCK)
        kext[pl.ds(at, BLOCK), :] = hot.astype(jnp.bfloat16)

    for i in range(blocks):
        row = docs_ref[i : i + 1, :]
        put_kext(i, row)
        same = jnp.where(column_of(row) == lanes_f, 0.0, -far_score)
        names = jnp.where(listed[i] > 0, 0.0, -far_score)
        qext[i] = jnp.where(is_doc, same, names).astype(jnp.bfloat16)

    def far_kext(d, carry):
        src = lax.rem(own - d + seq_count, seq_count)
        want = jnp.max(jnp.where(lane == src, asked, 0), axis=1, keepdims=True)
        want = jnp.maximum(want - 1, 0)
        note = note_in[d - 1]
        rows = lax.broadcasted_iota(jnp.int32, note.shape, 0)
        row = jnp.max(jnp.where(rows == want, note, 0), axis=0, keepdims=True)
        put_kext(blocks + d - 1, row)
        return carry

    lax.fori_loop(1, seq_count, far_kext, 0)
    loads[2].wait()

    ones = jnp.ones((BLOCK, LANES), jnp.bfloat16)

    def key_tile(s, h, which):
        if s < blocks:
            ref = v_ref if which else k_ref
            at = h * HEAD_SIZE
            if not isinstance(h, int):
                at = pl.multiple_of(at, HEAD_SIZE)
            return ref[s * BLOCK : (s + 1) * BLOCK, pl.ds(at, HEAD_SIZE)]
        return land[s - blocks, h, which * BLOCK : (which + 1) * BLOCK, :]

    chunks = [list(range(s, min(s + 2, slots))) for s in range(0, slots, 2)]
    parts = 2
    per = GROUP // parts

    def attend(h, i):
        at = pl.multiple_of(i * BLOCK, BLOCK)
        bias = qext[i]
        keys = [
            jnp.concatenate(
                [
                    jnp.concatenate(
                        [key_tile(s, h, 0), kext[s * BLOCK : (s + 1) * BLOCK, :]], axis=1
                    )
                    for s in chunk
                ],
                axis=0,
            )
            for chunk in chunks
        ]
        tops = []
        for part in range(parts):
            q = jnp.concatenate(
                [
                    jnp.concatenate(
                        [
                            q_ref[
                                pl.ds(at, BLOCK),
                                pl.ds(
                                    pl.multiple_of(
                                        h * width + (part * per + g) * HEAD_SIZE, HEAD_SIZE
                                    ),
                                    HEAD_SIZE,
                                ),
                            ],
                            bias,
                        ],
                        axis=1,
                    )
                    for g in range(per)
                ],
                axis=0,
            )
            top = None
            for chunk, k in zip(chunks, keys):
                s = lax.dot_general(
                    q, k, (((1,), (1,)), ((), ())), preferred_element_type=jnp.float32
                )
                for n, b in enumerate(chunk):
                    t = s[:, n * BLOCK : (n + 1) * BLOCK]
                    scores[part][:, b * BLOCK : (b + 1) * BLOCK] = t
                    top = t if top is None else jnp.maximum(top, t)
            tops.append(top)
        for part in range(parts):
            top = jnp.max(tops[part], axis=1, keepdims=True)
            for s in range(slots):
                here = slice(s * BLOCK, (s + 1) * BLOCK)
                probs[part][:, here] = jnp.exp2(
                    (scores[part][:, here] - top) * exp2_scale
                ).astype(jnp.bfloat16)
            v = jnp.concatenate(
                [jnp.concatenate([key_tile(s, h, 1), ones], axis=1) for s in range(slots)], axis=0
            )
            o = jnp.dot(probs[part][...], v, preferred_element_type=jnp.float32)
            o = (o[:, :HEAD_SIZE] / o[:, HEAD_SIZE:]).astype(jnp.bfloat16)
            for g in range(per):
                attn[
                    pl.ds(at, BLOCK),
                    pl.ds(
                        pl.multiple_of(h * width + (part * per + g) * HEAD_SIZE, HEAD_SIZE),
                        HEAD_SIZE,
                    ),
                ] = o[g * BLOCK : (g + 1) * BLOCK]

    def wait_head(h):
        def arrive(d, carry):
            kv_copy(d, h).wait_recv()
            return carry

        lax.fori_loop(1, seq_count, arrive, 0)

    def one_head(h, carry):
        wait_head(h)

        def one_row(i, inner):
            attend(h, i)
            return inner

        return lax.fori_loop(0, blocks, one_row, carry)

    lax.fori_loop(0, kv_heads - 1, one_head, 0)

    last = kv_heads - 1
    wait_head(last)

    def sent(n, carry):
        kv_copy(n // kv_heads + 1, lax.rem(n, kv_heads)).wait_send()
        return carry

    lax.fori_loop(0, (seq_count - 1) * kv_heads, sent, 0)

    @pl.when(core + 1 < dp_count)
    def _():
        pl.semaphore_signal(turn_sem, inc=1, device_id={"dp": core + 1}, device_id_type=MESH)

    loads[3].wait()

    def project(i, target, at, put):
        rows = attn[pl.ds(pl.multiple_of(i * BLOCK, BLOCK), BLOCK), :]
        for t in range(0, piece, tile):
            start = pl.multiple_of(target * cols + at + t, tile)
            put(
                t,
                jnp.dot(rows, w_ref[:, pl.ds(start, tile)], preferred_element_type=jnp.float32),
            )

    def y_copy(o, i, p):
        return pltpu.make_async_remote_copy(
            src_ref=ysend.at[o, i, p],
            dst_ref=yrecv.at[o, i, p],
            send_sem=y_ssem.at[o, i, p],
            recv_sem=y_rsem.at[o, i, p],
            device_id={"head": lax.rem(head + o + 1, head_count)},
            device_id_type=MESH,
        )

    per_row = others * PIECES

    def y_at(n):
        i = n // per_row
        rest = lax.rem(n, per_row)
        return rest // PIECES, i, lax.rem(rest, PIECES)

    def last_head(i, carry):
        attend(last, i)

        def share(n, inner):
            o, _, p = y_at(n)

            def put(t, x):
                ysend[o, i, p, :, t : t + tile] = x.astype(jnp.bfloat16)

            project(i, lax.rem(head + o + 1, head_count), p * piece, put)
            before = i * per_row + n - 1

            @pl.when(before >= 0)
            def _():
                y_copy(*y_at(before)).start()

            return inner

        return lax.fori_loop(0, per_row, share, carry)

    lax.fori_loop(0, blocks, last_head, 0)

    def own_share(n, carry):
        i = n // PIECES
        p = lax.rem(n, PIECES)
        rows = pl.ds(pl.multiple_of(i * BLOCK, BLOCK), BLOCK)

        def put(t, x):
            kept[rows, pl.ds(pl.multiple_of(p * piece + t, tile), tile)] = x

        project(i, head, p * piece, put)

        @pl.when(n == 0)
        def _():
            y_copy(*y_at(blocks * per_row - 1)).start()

        return carry

    lax.fori_loop(0, blocks * PIECES, own_share, 0)

    def out_copy(i):
        rows = pl.ds(pl.multiple_of(i * BLOCK, BLOCK), BLOCK)
        return pltpu.make_async_copy(done.at[rows, :], out_hbm.at[rows, :], out_sem.at[i])

    def finish(i, carry):
        rows = pl.ds(pl.multiple_of(i * BLOCK, BLOCK), BLOCK)
        for p in range(PIECES):
            total = kept[rows, p * piece : (p + 1) * piece]
            for o in range(others):
                y_copy(o, i, p).wait_recv()
                total = total + yrecv[o, i, p].astype(jnp.float32)
            done[rows, p * piece : (p + 1) * piece] = total.astype(jnp.bfloat16)
        out_copy(i).start()
        return carry

    lax.fori_loop(0, blocks, finish, 0)

    def drain(i, carry):
        for o in range(others):
            for p in range(PIECES):
                y_copy(o, i, p).wait_send()
        out_copy(i).wait()
        return carry

    lax.fori_loop(0, blocks, drain, 0)
    for d in range(1, seq_count):
        note_copy(d).wait_send()


def per_device(queries, keys, values, doc_ids, block_lists, w_out):
    tokens, depth = queries.shape
    blocks = tokens // BLOCK
    kv_width = keys.shape[1]
    kv_heads = kv_width // HEAD_SIZE
    seq_count = lax.axis_size("seq")
    head_count = lax.axis_size("head")
    dp_count = lax.axis_size("dp")
    far = seq_count - 1
    others = head_count - 1
    slots = blocks + far
    cols = w_out.shape[1] // head_count
    note_rows = -(-(blocks + 1) // 8) * 8
    assert DOCS + slots <= LANES
    hbm = pl.BlockSpec(memory_space=pl.ANY)
    bf16, f32, i32 = jnp.bfloat16, jnp.float32, jnp.int32
    half = GROUP // 2 * BLOCK
    return pl.pallas_call(
        functools.partial(kernel, seq_count, head_count, dp_count),
        out_shape=jax.ShapeDtypeStruct((tokens, cols), bf16),
        in_specs=[
            pl.BlockSpec(memory_space=pltpu.SMEM),
            pl.BlockSpec(memory_space=pltpu.VMEM),
            hbm,
            hbm,
            hbm,
            hbm,
        ],
        out_specs=hbm,
        scratch_shapes=[
            pltpu.VMEM((tokens, depth), bf16),
            pltpu.VMEM((tokens, kv_width), bf16),
            pltpu.VMEM((tokens, kv_width), bf16),
            pltpu.VMEM(w_out.shape, bf16),
            pltpu.VMEM((note_rows, LANES), i32),
            pltpu.VMEM((far, note_rows, LANES), i32),
            pltpu.VMEM((far, kv_heads, 2 * BLOCK, HEAD_SIZE), bf16),
            pltpu.VMEM((far, kv_heads, 2 * BLOCK, HEAD_SIZE), bf16),
            pltpu.VMEM((blocks, BLOCK, LANES), bf16),
            pltpu.VMEM((slots * BLOCK, LANES), bf16),
            [pltpu.VMEM((half, slots * BLOCK), f32) for _ in range(2)],
            [pltpu.VMEM((half, slots * BLOCK), bf16) for _ in range(2)],
            pltpu.VMEM((tokens, depth), bf16),
            pltpu.VMEM((others, blocks, PIECES, BLOCK, cols // PIECES), bf16),
            pltpu.VMEM((others, blocks, PIECES, BLOCK, cols // PIECES), bf16),
            pltpu.VMEM((tokens, cols), f32),
            pltpu.VMEM((tokens, cols), bf16),
            pltpu.SemaphoreType.DMA((4,)),
            pltpu.SemaphoreType.DMA((far,)),
            pltpu.SemaphoreType.DMA((far,)),
            pltpu.SemaphoreType.DMA((far, kv_heads)),
            pltpu.SemaphoreType.DMA((far, kv_heads)),
            pltpu.SemaphoreType.DMA((others, blocks, PIECES)),
            pltpu.SemaphoreType.DMA((others, blocks, PIECES)),
            pltpu.SemaphoreType.DMA((blocks,)),
            pltpu.SemaphoreType.REGULAR,
        ],
        compiler_params=pltpu.CompilerParams(
            collective_id=0, has_side_effects=True, vmem_limit_bytes=62 * 2**20
        ),
    )(block_lists, doc_ids.reshape(blocks, BLOCK), queries, keys, values, w_out)


def solution(mesh):
    in_specs = (
        P(("dp", "seq"), "head"),
        P(("dp", "seq"), "head"),
        P(("dp", "seq"), "head"),
        P(("dp", "seq")),
        P(("dp", "seq"), None),
        P("head", None),
    )
    out_specs = P(("dp", "seq"), "head")
    return jax.shard_map(
        per_device, mesh=mesh, in_specs=in_specs, out_specs=out_specs, check_vma=False
    )
```

```python
import functools
import math

import jax
import jax.numpy as jnp
from jax import lax
from jax.experimental import pallas as pl
from jax.experimental.pallas import tpu as pltpu
from jax.sharding import PartitionSpec as P

HEAD_SIZE = 128
BLOCK = 128
LANES = 128
DOCS = 8
GROUP = 4
PIECES = 4
TILE = 512
MESH = pl.DeviceIdType.MESH

far_score = float(2**20)
exp2_scale = math.log2(math.e) / math.sqrt(HEAD_SIZE)


def column_of(row):
    return jnp.broadcast_to(row, (BLOCK, LANES)).astype(jnp.float32).T


def kernel(
    seq_count,
    head_count,
    dp_count,
    lists_hbm,
    docs_hbm,
    q_hbm,
    k_hbm,
    v_hbm,
    w_hbm,
    out_ref,
    lists_ref,
    docs_ref,
    q_ref,
    k_ref,
    v_ref,
    w_ref,
    note_out,
    note_in,
    stage,
    land,
    qext,
    kext,
    scores,
    probs,
    attn,
    ysend,
    yrecv,
    kept,
    own_sum,
    own_top,
    load_sem,
    note_ssem,
    note_rsem,
    kv_ssem,
    kv_rsem,
    y_ssem,
    y_rsem,
    turn_sem,
):
    own = lax.axis_index("seq")
    head = lax.axis_index("head")
    core = lax.axis_index("dp")
    blocks = docs_ref.shape[0]
    slots = blocks + seq_count - 1
    kv_heads = k_ref.shape[1] // HEAD_SIZE
    width = GROUP * HEAD_SIZE
    cols = kept.shape[1]
    piece = cols // PIECES
    tile = min(TILE, piece)
    others = head_count - 1

    loads = [
        pltpu.make_async_copy(src, dst, load_sem.at[n])
        for n, (src, dst) in enumerate(
            (
                (docs_hbm, docs_ref),
                (lists_hbm, lists_ref),
                (k_hbm, k_ref),
                (v_hbm, v_ref),
                (q_hbm, q_ref),
                (w_hbm, w_ref),
            )
        )
    ]
    for load in loads:
        load.start()

    barrier = pltpu.get_barrier_semaphore()
    for d in range(1, seq_count):
        pl.semaphore_signal(
            barrier, inc=1, device_id={"seq": lax.rem(own + d, seq_count)}, device_id_type=MESH
        )
    for d in range(1, head_count):
        pl.semaphore_signal(
            barrier, inc=1, device_id={"head": lax.rem(head + d, head_count)}, device_id_type=MESH
        )
    for d in range(1, dp_count):
        pl.semaphore_signal(
            barrier, inc=1, device_id={"dp": lax.rem(core + d, dp_count)}, device_id_type=MESH
        )

    loads[0].wait()
    loads[1].wait()

    lane = lax.broadcasted_iota(jnp.int32, (1, LANES), 1)
    slot = lane - DOCS
    source = own - (slot - blocks + 1)
    source = jnp.where(source < 0, source + seq_count, source)
    is_own = (slot >= 0) & (slot < blocks)
    is_far = (slot >= blocks) & (slot < slots)
    low = jnp.where(is_own, own * blocks + slot, jnp.where(is_far, source * blocks, -1))
    high = jnp.where(is_own, low + 1, jnp.where(is_far, low + blocks, -1))
    owner_low = lane * blocks
    asked = jnp.zeros((1, LANES), jnp.int32)
    listed = []
    for i in range(blocks):
        here = jnp.zeros((1, LANES), jnp.int32)
        for j in range(lists_ref.shape[1]):
            block = lists_ref[i, j]
            here = jnp.where((block >= low) & (block < high), 1, here)
            inside = (block >= owner_low) & (block < owner_low + blocks)
            asked = jnp.maximum(asked, jnp.where(inside, block - owner_low + 1, 0))
        listed.append(here)
    note_out[0:blocks, :] = docs_ref[...]
    note_out[blocks : blocks + 1, :] = asked

    pl.semaphore_wait(barrier, seq_count + head_count + dp_count - 3)

    def note_copy(d):
        return pltpu.make_async_remote_copy(
            src_ref=note_out,
            dst_ref=note_in.at[d - 1],
            send_sem=note_ssem.at[d - 1],
            recv_sem=note_rsem.at[d - 1],
            device_id={"seq": lax.rem(own + d, seq_count)},
            device_id_type=MESH,
        )

    def kv_copy(d, h):
        return pltpu.make_async_remote_copy(
            src_ref=stage.at[d - 1, h],
            dst_ref=land.at[d - 1, h],
            send_sem=kv_ssem.at[d - 1, h],
            recv_sem=kv_rsem.at[d - 1, h],
            device_id={"seq": lax.rem(own + d, seq_count)},
            device_id_type=MESH,
        )

    def step_of(n):
        near = n // 2 + 1
        return jnp.where(lax.rem(n, 2) == 0, near, seq_count - near)

    for d in range(1, seq_count):
        note_copy(d).start()
    loads[2].wait()
    loads[3].wait()
    loads[4].wait()

    def send_heads(first):
        def send_head(h, carry):
            def send(n, inner):
                kv_copy(step_of(n), h).start()
                return inner

            return lax.fori_loop(0, seq_count - 1, send, carry)

        lax.fori_loop(first, kv_heads, send_head, 0)

    lanes = lax.broadcasted_iota(jnp.int32, (BLOCK, LANES), 1)
    lanes_f = lanes.astype(jnp.float32)
    is_doc = lanes < DOCS

    def put_kext(s, row):
        same = jnp.where(column_of(row) == lanes_f, 1.0, 0.0)
        hot = jnp.where(is_doc, same, jnp.where(lanes == DOCS + s, 1.0, 0.0))
        at = s * BLOCK
        if not isinstance(s, int):
            at = pl.multiple_of(at, BLOCK)
        kext[pl.ds(at, BLOCK), :] = hot.astype(jnp.bfloat16)

    for i in range(blocks):
        row = docs_ref[i : i + 1, :]
        put_kext(i, row)
        same = jnp.where(column_of(row) == lanes_f, 0.0, -far_score)
        names = jnp.where(listed[i] > 0, 0.0, -far_score)
        qext[i] = jnp.where(is_doc, same, names).astype(jnp.bfloat16)

    def far_kext():
        for d in range(1, seq_count):
            src = lax.rem(own - d + seq_count, seq_count)
            want = jnp.max(jnp.where(lane == src, asked, 0), axis=1, keepdims=True)
            want = jnp.maximum(want - 1, 0)
            note = note_in[d - 1]
            rows = lax.broadcasted_iota(jnp.int32, note.shape, 0)
            row = jnp.max(jnp.where(rows == want, note, 0), axis=0, keepdims=True)
            put_kext(blocks + d - 1, row)

    ones = jnp.ones((BLOCK, LANES), jnp.bfloat16)

    def key_tile(s, h, which):
        if s < blocks:
            ref = v_ref if which else k_ref
            at = h * HEAD_SIZE
            if not isinstance(h, int):
                at = pl.multiple_of(at, HEAD_SIZE)
            return ref[s * BLOCK : (s + 1) * BLOCK, pl.ds(at, HEAD_SIZE)]
        return land[s - blocks, h, which * BLOCK : (which + 1) * BLOCK, :]

    parts = 2
    per = GROUP // parts
    part_rows = per * BLOCK

    def softmax_sums(h, i, names):
        at = pl.multiple_of(i * BLOCK, BLOCK)
        bias = qext[i]
        chunks = [names[n : n + 2] for n in range(0, len(names), 2)]
        keys = [
            jnp.concatenate(
                [
                    jnp.concatenate(
                        [key_tile(s, h, 0), kext[s * BLOCK : (s + 1) * BLOCK, :]], axis=1
                    )
                    for s in chunk
                ],
                axis=0,
            )
            for chunk in chunks
        ]
        v = jnp.concatenate(
            [jnp.concatenate([key_tile(s, h, 1), ones], axis=1) for s in names], axis=0
        )
        tops = []
        for part in range(parts):
            q = jnp.concatenate(
                [
                    jnp.concatenate([q_ref[pl.ds(at, BLOCK), head_cols(h, part * per + g)], bias], axis=1)
                    for g in range(per)
                ],
                axis=0,
            )
            top = None
            n = 0
            for k in keys:
                s = lax.dot_general(
                    q, k, (((1,), (1,)), ((), ())), preferred_element_type=jnp.float32
                )
                for m in range(k.shape[0] // BLOCK):
                    t = s[:, m * BLOCK : (m + 1) * BLOCK]
                    scores[part][:, n * BLOCK : (n + 1) * BLOCK] = t
                    top = t if top is None else jnp.maximum(top, t)
                    n += 1
            tops.append(top)
        found = []
        for part in range(parts):
            top = jnp.max(tops[part], axis=1, keepdims=True)
            for n in range(len(names)):
                here = slice(n * BLOCK, (n + 1) * BLOCK)
                probs[part][:, here] = jnp.exp2(
                    (scores[part][:, here] - top) * exp2_scale
                ).astype(jnp.bfloat16)
            o = jnp.dot(
                probs[part][:, : len(names) * BLOCK], v, preferred_element_type=jnp.float32
            )
            found.append((top, o))
        return found

    def head_cols(h, g):
        return pl.ds(pl.multiple_of(h * width + g * HEAD_SIZE, HEAD_SIZE), HEAD_SIZE)

    own_slots = list(range(blocks))
    far_slots = list(range(blocks, slots))

    def attend_own(n, carry):
        found = softmax_sums(n // blocks, lax.rem(n, blocks), own_slots)
        for part, (top, o) in enumerate(found):
            own_top[n, part] = jnp.broadcast_to(top, (part_rows, LANES))
            own_sum[n, part] = o
        return carry

    def attend(h, i):
        at = pl.multiple_of(i * BLOCK, BLOCK)
        n = h * blocks + i
        for part, (top, o) in enumerate(softmax_sums(h, i, far_slots)):
            first = own_top[n, part]
            both = jnp.maximum(first, top)
            near = jnp.exp2((first - both) * exp2_scale)
            far = jnp.exp2((top - both) * exp2_scale)
            x = own_sum[n, part]
            total = x[:, :HEAD_SIZE] * near + o[:, :HEAD_SIZE] * far
            count = x[:, HEAD_SIZE:] * near + o[:, HEAD_SIZE:] * far
            result = (total / count).astype(jnp.bfloat16)
            for g in range(per):
                attn[pl.ds(at, BLOCK), head_cols(h, part * per + g)] = result[
                    g * BLOCK : (g + 1) * BLOCK
                ]

    def fill(n, carry):
        d = step_of(n)
        note_copy(seq_count - d).wait_recv()
        row = note_in[seq_count - d - 1, blocks : blocks + 1, :]
        want = jnp.max(jnp.where(lane == own, row, 0), axis=1, keepdims=True)
        want = jnp.broadcast_to(jnp.maximum(want - 1, 0), (BLOCK, LANES))
        hots = [jnp.where(want == b, 1.0, 0.0).astype(jnp.bfloat16) for b in range(blocks)]
        for h in range(kv_heads):
            cut = slice(h * HEAD_SIZE, (h + 1) * HEAD_SIZE)
            for part, ref in enumerate((k_ref, v_ref)):
                picked = None
                for b in range(blocks):
                    term = ref[b * BLOCK : (b + 1) * BLOCK, cut] * hots[b]
                    picked = term if picked is None else picked + term
                stage[d - 1, h, part * BLOCK : (part + 1) * BLOCK, :] = picked

        @pl.when(core == 0)
        def _():
            for h in range(early):
                kv_copy(d, h).start()

        @pl.when(n < kv_heads * blocks)
        def _():
            attend_own(n, 0)

        return carry

    early = min(2, kv_heads)
    lax.fori_loop(0, seq_count - 1, fill, 0)

    @pl.when(core == 0)
    def _():
        send_heads(early)

    lax.fori_loop(min(seq_count - 1, kv_heads * blocks), kv_heads * blocks, attend_own, 0)

    @pl.when(core > 0)
    def _():
        pl.semaphore_wait(turn_sem, 1)
        send_heads(0)

    far_kext()

    def wait_head(h):
        def arrive(d, carry):
            kv_copy(d, h).wait_recv()
            return carry

        lax.fori_loop(1, seq_count, arrive, 0)

    def one_head(h, carry):
        wait_head(h)

        def one_row(i, inner):
            attend(h, i)
            return inner

        return lax.fori_loop(0, blocks, one_row, carry)

    lax.fori_loop(0, kv_heads - 1, one_head, 0)

    @pl.when(core + 1 < dp_count)
    def _():
        pl.semaphore_signal(turn_sem, inc=1, device_id={"dp": core + 1}, device_id_type=MESH)

    last = kv_heads - 1
    wait_head(last)
    loads[5].wait()

    def project(i, target, at, put):
        rows = attn[pl.ds(pl.multiple_of(i * BLOCK, BLOCK), BLOCK), :]
        for t in range(0, piece, tile):
            start = pl.multiple_of(target * cols + at + t, tile)
            put(
                t,
                jnp.dot(rows, w_ref[:, pl.ds(start, tile)], preferred_element_type=jnp.float32),
            )

    def y_copy(o, i, p):
        return pltpu.make_async_remote_copy(
            src_ref=ysend.at[o, i, p],
            dst_ref=yrecv.at[o, i, p],
            send_sem=y_ssem.at[o, i, p],
            recv_sem=y_rsem.at[o, i, p],
            device_id={"head": lax.rem(head + o + 1, head_count)},
            device_id_type=MESH,
        )

    per_row = others * PIECES

    def y_at(n):
        i = n // per_row
        rest = lax.rem(n, per_row)
        return rest // PIECES, i, lax.rem(rest, PIECES)

    def last_head(i, carry):
        attend(last, i)

        def share(n, inner):
            o, _, p = y_at(n)

            def put(t, x):
                ysend[o, i, p, :, t : t + tile] = x.astype(jnp.bfloat16)

            project(i, lax.rem(head + o + 1, head_count), p * piece, put)
            before = i * per_row + n - 1

            @pl.when(before >= 0)
            def _():
                y_copy(*y_at(before)).start()

            return inner

        return lax.fori_loop(0, per_row, share, carry)

    lax.fori_loop(0, blocks, last_head, 0)

    def own_share(n, carry):
        i = n // PIECES
        p = lax.rem(n, PIECES)
        rows = pl.ds(pl.multiple_of(i * BLOCK, BLOCK), BLOCK)

        def put(t, x):
            kept[rows, pl.ds(pl.multiple_of(p * piece + t, tile), tile)] = x

        project(i, head, p * piece, put)

        @pl.when(n == 0)
        def _():
            y_copy(*y_at(blocks * per_row - 1)).start()

        return carry

    lax.fori_loop(0, blocks * PIECES, own_share, 0)

    for d in range(1, seq_count):
        note_copy(d).wait_send()

    def sent(n, carry):
        kv_copy(n // kv_heads + 1, lax.rem(n, kv_heads)).wait_send()
        return carry

    lax.fori_loop(0, (seq_count - 1) * kv_heads, sent, 0)

    def finish(i, carry):
        rows = pl.ds(pl.multiple_of(i * BLOCK, BLOCK), BLOCK)
        for p in range(PIECES):
            total = kept[rows, p * piece : (p + 1) * piece]
            for o in range(others):
                y_copy(o, i, p).wait_recv()
                total = total + yrecv[o, i, p].astype(jnp.float32)
            out_ref[rows, p * piece : (p + 1) * piece] = total.astype(jnp.bfloat16)
            for o in range(others):
                y_copy(o, i, p).wait_send()
        return carry

    lax.fori_loop(0, blocks, finish, 0)


def per_device(queries, keys, values, doc_ids, block_lists, w_out):
    tokens, depth = queries.shape
    blocks = tokens // BLOCK
    kv_width = keys.shape[1]
    kv_heads = kv_width // HEAD_SIZE
    seq_count = lax.axis_size("seq")
    head_count = lax.axis_size("head")
    dp_count = lax.axis_size("dp")
    far = seq_count - 1
    others = head_count - 1
    slots = blocks + far
    cols = w_out.shape[1] // head_count
    note_rows = -(-(blocks + 1) // 8) * 8
    assert DOCS + slots <= LANES
    hbm = pl.BlockSpec(memory_space=pl.ANY)
    bf16, f32, i32 = jnp.bfloat16, jnp.float32, jnp.int32
    half = GROUP // 2 * BLOCK
    return pl.pallas_call(
        functools.partial(kernel, seq_count, head_count, dp_count),
        out_shape=jax.ShapeDtypeStruct((tokens, cols), bf16),
        in_specs=[
            hbm,
        ]
        * 6,
        out_specs=pl.BlockSpec(memory_space=pltpu.VMEM),
        scratch_shapes=[
            pltpu.SMEM(block_lists.shape, i32),
            pltpu.VMEM((blocks, BLOCK), i32),
            pltpu.VMEM((tokens, depth), bf16),
            pltpu.VMEM((tokens, kv_width), bf16),
            pltpu.VMEM((tokens, kv_width), bf16),
            pltpu.VMEM(w_out.shape, bf16),
            pltpu.VMEM((note_rows, LANES), i32),
            pltpu.VMEM((far, note_rows, LANES), i32),
            pltpu.VMEM((far, kv_heads, 2 * BLOCK, HEAD_SIZE), bf16),
            pltpu.VMEM((far, kv_heads, 2 * BLOCK, HEAD_SIZE), bf16),
            pltpu.VMEM((blocks, BLOCK, LANES), bf16),
            pltpu.VMEM((slots * BLOCK, LANES), bf16),
            [pltpu.VMEM((half, max(blocks, far) * BLOCK), f32) for _ in range(2)],
            [pltpu.VMEM((half, max(blocks, far) * BLOCK), bf16) for _ in range(2)],
            pltpu.VMEM((tokens, depth), bf16),
            pltpu.VMEM((others, blocks, PIECES, BLOCK, cols // PIECES), bf16),
            pltpu.VMEM((others, blocks, PIECES, BLOCK, cols // PIECES), bf16),
            pltpu.VMEM((tokens, cols), f32),
            pltpu.VMEM((kv_heads * blocks, 2, half, 2 * LANES), f32),
            pltpu.VMEM((kv_heads * blocks, 2, half, LANES), f32),
            pltpu.SemaphoreType.DMA((6,)),
            pltpu.SemaphoreType.DMA((far,)),
            pltpu.SemaphoreType.DMA((far,)),
            pltpu.SemaphoreType.DMA((far, kv_heads)),
            pltpu.SemaphoreType.DMA((far, kv_heads)),
            pltpu.SemaphoreType.DMA((others, blocks, PIECES)),
            pltpu.SemaphoreType.DMA((others, blocks, PIECES)),
            pltpu.SemaphoreType.REGULAR,
        ],
        compiler_params=pltpu.CompilerParams(
            collective_id=0, has_side_effects=True, vmem_limit_bytes=51500 * 2**10
        ),
    )(
        *[
            pltpu.with_memory_space_constraint(x, pltpu.HBM)
            for x in (
                block_lists,
                doc_ids.reshape(blocks, BLOCK),
                queries,
                keys,
                values,
                w_out,
            )
        ]
    )


def solution(mesh):
    in_specs = (
        P(("dp", "seq"), "head"),
        P(("dp", "seq"), "head"),
        P(("dp", "seq"), "head"),
        P(("dp", "seq")),
        P(("dp", "seq"), None),
        P("head", None),
    )
    out_specs = P(("dp", "seq"), "head")
    return jax.shard_map(
        per_device, mesh=mesh, in_specs=in_specs, out_specs=out_specs, check_vma=False
    )
```

```python
import functools
import math

import jax
import jax.numpy as jnp
from jax import lax
from jax.experimental import pallas as pl
from jax.experimental.pallas import tpu as pltpu
from jax.sharding import PartitionSpec as P

HEAD_SIZE = 128
BLOCK = 128
LANES = 128
DOCS = 8
GROUP = 4
PIECES = 4
TILE = 1024
MESH = pl.DeviceIdType.MESH

far_score = float(2**20)
exp2_scale = math.log2(math.e) / math.sqrt(HEAD_SIZE)


def column_of(row):
    return jnp.broadcast_to(row, (BLOCK, LANES)).astype(jnp.float32).T


def kernel(
    seq_count,
    head_count,
    dp_count,
    lists_hbm,
    docs_hbm,
    q_hbm,
    k_hbm,
    v_hbm,
    w_hbm,
    out_ref,
    lists_ref,
    docs_ref,
    q_ref,
    k_ref,
    v_ref,
    w_ref,
    note_out,
    note_in,
    stage,
    land,
    qext,
    kext,
    scores,
    probs,
    attn,
    ysend,
    yrecv,
    kept,
    own_sum,
    own_top,
    load_sem,
    note_ssem,
    note_rsem,
    kv_ssem,
    kv_rsem,
    y_ssem,
    y_rsem,
    turn_sem,
):
    own = lax.axis_index("seq")
    head = lax.axis_index("head")
    core = lax.axis_index("dp")
    blocks = docs_ref.shape[0]
    slots = blocks + seq_count - 1
    kv_heads = k_ref.shape[1] // HEAD_SIZE
    width = GROUP * HEAD_SIZE
    cols = kept.shape[1]
    pieces = ysend.shape[2]
    piece = cols // pieces
    tile = math.gcd(TILE, cols)
    own_tiles = cols // tile
    others = head_count - 1

    loads = [
        pltpu.make_async_copy(src, dst, load_sem.at[n])
        for n, (src, dst) in enumerate(
            (
                (docs_hbm, docs_ref),
                (lists_hbm, lists_ref),
                (k_hbm, k_ref),
                (v_hbm, v_ref),
                (q_hbm, q_ref),
                (w_hbm, w_ref),
            )
        )
    ]
    for load in loads:
        load.start()

    barrier = pltpu.get_barrier_semaphore()
    for d in range(1, seq_count):
        pl.semaphore_signal(
            barrier, inc=1, device_id={"seq": lax.rem(own + d, seq_count)}, device_id_type=MESH
        )
    for d in range(1, head_count):
        pl.semaphore_signal(
            barrier, inc=1, device_id={"head": lax.rem(head + d, head_count)}, device_id_type=MESH
        )
    for d in range(1, dp_count):
        pl.semaphore_signal(
            barrier, inc=1, device_id={"dp": lax.rem(core + d, dp_count)}, device_id_type=MESH
        )

    loads[0].wait()
    loads[1].wait()

    lane = lax.broadcasted_iota(jnp.int32, (1, LANES), 1)
    slot = lane - DOCS
    source = own - (slot - blocks + 1)
    source = jnp.where(source < 0, source + seq_count, source)
    is_own = (slot >= 0) & (slot < blocks)
    is_far = (slot >= blocks) & (slot < slots)
    low = jnp.where(is_own, own * blocks + slot, jnp.where(is_far, source * blocks, -1))
    high = jnp.where(is_own, low + 1, jnp.where(is_far, low + blocks, -1))
    owner_low = lane * blocks
    asked = jnp.zeros((1, LANES), jnp.int32)
    listed = []
    for i in range(blocks):
        here = jnp.zeros((1, LANES), jnp.int32)
        for j in range(lists_ref.shape[1]):
            block = lists_ref[i, j]
            here = jnp.where((block >= low) & (block < high), 1, here)
            inside = (block >= owner_low) & (block < owner_low + blocks)
            asked = jnp.maximum(asked, jnp.where(inside, block - owner_low + 1, 0))
        listed.append(here)
    note_out[0:blocks, :] = docs_ref[...]
    note_out[blocks : blocks + 1, :] = asked

    pl.semaphore_wait(barrier, seq_count + head_count + dp_count - 3)

    def note_copy(d):
        return pltpu.make_async_remote_copy(
            src_ref=note_out,
            dst_ref=note_in.at[d - 1],
            send_sem=note_ssem.at[d - 1],
            recv_sem=note_rsem.at[d - 1],
            device_id={"seq": lax.rem(own + d, seq_count)},
            device_id_type=MESH,
        )

    def kv_copy(d, h):
        return pltpu.make_async_remote_copy(
            src_ref=stage.at[d - 1, h],
            dst_ref=land.at[d - 1, h],
            send_sem=kv_ssem.at[d - 1, h],
            recv_sem=kv_rsem.at[d - 1, h],
            device_id={"seq": lax.rem(own + d, seq_count)},
            device_id_type=MESH,
        )

    sides = jnp.minimum(own, seq_count - 1 - own)

    def step_of(n):
        pair = n // 2 + 1
        rest = n - sides + 1
        both = jnp.where(lax.rem(n, 2) == 0, pair, seq_count - pair)
        one = jnp.where(own < seq_count - 1 - own, rest, seq_count - rest)
        return jnp.where(n < 2 * sides, both, one)

    for d in range(1, seq_count):
        note_copy(d).start()
    loads[2].wait()
    loads[3].wait()

    def send_heads(first):
        def send_head(h, carry):
            def send(n, inner):
                kv_copy(step_of(seq_count - 2 - n), h).start()
                return inner

            return lax.fori_loop(0, seq_count - 1, send, carry)

        lax.fori_loop(first, kv_heads, send_head, 0)

    lanes = lax.broadcasted_iota(jnp.int32, (BLOCK, LANES), 1)
    lanes_f = lanes.astype(jnp.float32)
    is_doc = lanes < DOCS

    def put_kext(s, row):
        same = jnp.where(column_of(row) == lanes_f, 1.0, 0.0)
        hot = jnp.where(is_doc, same, jnp.where(lanes == DOCS + s, 1.0, 0.0))
        at = s * BLOCK
        if not isinstance(s, int):
            at = pl.multiple_of(at, BLOCK)
        kext[pl.ds(at, BLOCK), :] = hot.astype(jnp.bfloat16)

    for i in range(blocks):
        row = docs_ref[i : i + 1, :]
        put_kext(i, row)
        same = jnp.where(column_of(row) == lanes_f, 0.0, -far_score)
        names = jnp.where(listed[i] > 0, 0.0, -far_score)
        qext[i] = jnp.where(is_doc, same, names).astype(jnp.bfloat16)

    def far_kext():
        for d in range(1, seq_count):
            src = lax.rem(own - d + seq_count, seq_count)
            want = jnp.max(jnp.where(lane == src, asked, 0), axis=1, keepdims=True)
            want = jnp.maximum(want - 1, 0)
            note = note_in[d - 1]
            rows = lax.broadcasted_iota(jnp.int32, note.shape, 0)
            row = jnp.max(jnp.where(rows == want, note, 0), axis=0, keepdims=True)
            put_kext(blocks + d - 1, row)

    ones = jnp.ones((BLOCK, LANES), jnp.bfloat16)

    def key_tile(s, h, which):
        if s < blocks:
            ref = v_ref if which else k_ref
            at = h * HEAD_SIZE
            if not isinstance(h, int):
                at = pl.multiple_of(at, HEAD_SIZE)
            return ref[s * BLOCK : (s + 1) * BLOCK, pl.ds(at, HEAD_SIZE)]
        return land[s - blocks, h, which * BLOCK : (which + 1) * BLOCK, :]

    parts = 2
    per = GROUP // parts
    part_rows = per * BLOCK

    def softmax_sums(h, rows, names, put):
        chunks = [names[n : n + 2] for n in range(0, len(names), 2)]
        keys = [
            jnp.concatenate(
                [
                    jnp.concatenate(
                        [key_tile(s, h, 0), kext[s * BLOCK : (s + 1) * BLOCK, :]], axis=1
                    )
                    for s in chunk
                ],
                axis=0,
            )
            for chunk in chunks
        ]
        v = jnp.concatenate(
            [jnp.concatenate([key_tile(s, h, 1), ones], axis=1) for s in names], axis=0
        )
        units = [(i, part) for i in rows for part in range(parts)]

        def score(u):
            i, part = units[u]
            at = pl.multiple_of(i * BLOCK, BLOCK)
            bias = qext[i]
            q = jnp.concatenate(
                [
                    jnp.concatenate(
                        [q_ref[pl.ds(at, BLOCK), head_cols(h, part * per + g)], bias], axis=1
                    )
                    for g in range(per)
                ],
                axis=0,
            )
            top = None
            n = 0
            for k in keys:
                s = lax.dot_general(
                    q, k, (((1,), (1,)), ((), ())), preferred_element_type=jnp.float32
                )
                for m in range(k.shape[0] // BLOCK):
                    t = s[:, m * BLOCK : (m + 1) * BLOCK]
                    scores[u % 2][:, n * BLOCK : (n + 1) * BLOCK] = t
                    top = t if top is None else jnp.maximum(top, t)
                    n += 1
            return top

        top = score(0)
        for u, (i, part) in enumerate(units):
            later = score(u + 1) if u + 1 < len(units) else None
            top = jnp.max(top, axis=1, keepdims=True)
            for n in range(len(names)):
                here = slice(n * BLOCK, (n + 1) * BLOCK)
                probs[u % 2][:, here] = jnp.exp2(
                    (scores[u % 2][:, here] - top) * exp2_scale
                ).astype(jnp.bfloat16)
            o = jnp.dot(
                probs[u % 2][:, : len(names) * BLOCK], v, preferred_element_type=jnp.float32
            )
            put(i, part, top, o)
            top = later

    def head_cols(h, g):
        return pl.ds(pl.multiple_of(h * width + g * HEAD_SIZE, HEAD_SIZE), HEAD_SIZE)

    own_slots = list(range(blocks))
    far_slots = list(range(blocks, slots))

    span = math.gcd(blocks, 2)
    steps = blocks // span

    def rows_of(n):
        return [n * span + r for r in range(span)]

    def attend_own(n, carry):
        h = n // steps

        def put(i, part, top, o):
            own_top[h * blocks + i, part] = jnp.broadcast_to(top, (part_rows, LANES))
            own_sum[h * blocks + i, part] = o

        softmax_sums(h, rows_of(lax.rem(n, steps)), own_slots, put)
        return carry

    def attend(h, rows):
        def put(i, part, top, o):
            at = pl.multiple_of(i * BLOCK, BLOCK)
            n = h * blocks + i
            first = own_top[n, part]
            both = jnp.maximum(first, top)
            near = jnp.exp2((first - both) * exp2_scale)
            far = jnp.exp2((top - both) * exp2_scale)
            x = own_sum[n, part]
            total = x[:, :HEAD_SIZE] * near + o[:, :HEAD_SIZE] * far
            count = x[:, HEAD_SIZE:] * near + o[:, HEAD_SIZE:] * far
            result = (total / count).astype(jnp.bfloat16)
            for g in range(per):
                attn[pl.ds(at, BLOCK), head_cols(h, part * per + g)] = result[
                    g * BLOCK : (g + 1) * BLOCK
                ]

        softmax_sums(h, rows, far_slots, put)

    def fill(n, carry):
        d = step_of(n)
        note_copy(seq_count - d).wait_recv()
        row = note_in[seq_count - d - 1, blocks : blocks + 1, :]
        want = jnp.max(jnp.where(lane == own, row, 0), axis=1, keepdims=True)
        want = jnp.broadcast_to(jnp.maximum(want - 1, 0), (BLOCK, LANES))
        hots = [jnp.where(want == b, 1.0, 0.0).astype(jnp.bfloat16) for b in range(blocks)]
        for h in range(kv_heads):
            cut = slice(h * HEAD_SIZE, (h + 1) * HEAD_SIZE)
            for part, ref in enumerate((k_ref, v_ref)):
                picked = None
                for b in range(blocks):
                    term = ref[b * BLOCK : (b + 1) * BLOCK, cut] * hots[b]
                    picked = term if picked is None else picked + term
                stage[d - 1, h, part * BLOCK : (part + 1) * BLOCK, :] = picked

        @pl.when(core == 0)
        def _():
            kv_copy(d, 0).start()

        return carry

    own_steps = kv_heads * steps
    lax.fori_loop(0, seq_count - 1, fill, 0)

    @pl.when(core == 0)
    def _():
        send_heads(1)

    loads[4].wait()
    lax.fori_loop(0, own_steps, attend_own, 0)

    @pl.when(core > 0)
    def _():
        pl.semaphore_wait(turn_sem, 1)
        send_heads(0)

    far_kext()

    def wait_head(h):
        def arrive(d, carry):
            kv_copy(d, h).wait_recv()
            return carry

        lax.fori_loop(1, seq_count, arrive, 0)

    def one_head(h, carry):
        wait_head(h)

        def one_row(i, inner):
            attend(h, rows_of(i))
            return inner

        return lax.fori_loop(0, steps, one_row, carry)

    last = kv_heads - 1
    before_last = max(last - 1, 0)
    lax.fori_loop(0, before_last, one_head, 0)
    for h in range(before_last, last):
        wait_head(h)
        attend(h, [0])

    @pl.when(core + 1 < dp_count)
    def _():
        pl.semaphore_signal(turn_sem, inc=1, device_id={"dp": core + 1}, device_id_type=MESH)

    wait_head(last)
    loads[5].wait()

    def project(i, target, at, size, put):
        rows = attn[pl.ds(pl.multiple_of(i * BLOCK, BLOCK), BLOCK), :]
        start = pl.multiple_of(target * cols + at, size)
        put(jnp.dot(rows, w_ref[:, pl.ds(start, size)], preferred_element_type=jnp.float32))

    def y_copy(o, i, p):
        return pltpu.make_async_remote_copy(
            src_ref=ysend.at[o, i, p],
            dst_ref=yrecv.at[o, i, p],
            send_sem=y_ssem.at[o, i, p],
            recv_sem=y_rsem.at[o, i, p],
            device_id={"head": lax.rem(head + o + 1, head_count)},
            device_id_type=MESH,
        )

    def share(i, size):
        groups = [
            (o, range(p, min(p + size, pieces)))
            for o in range(others)
            for p in range(0, pieces, size)
        ]
        for n, (o, group) in enumerate(groups):
            target = lax.rem(head + o + 1, head_count)

            def put(x):
                for p in group:
                    at = (p - group[0]) * piece
                    ysend[o, i, p] = x[:, at : at + piece].astype(jnp.bfloat16)

            project(i, target, group[0] * piece, len(group) * piece, put)
            if n > 0:
                for p in groups[n - 1][1]:
                    y_copy(groups[n - 1][0], i, p).start()
        return groups[-1]

    def send_rest(i, group):
        for p in group[1]:
            y_copy(group[0], i, p).start()

    def tail_row(i, carry):
        for h in range(before_last, last):
            attend(h, [i])

        @pl.when(i == 1)
        def _():
            send_rest(0, first_rest)

        @pl.when(i > 1)
        def _():
            send_rest(i - 1, rest)

        attend(last, [i])
        share(i, 2)
        return carry

    attend(last, [0])
    first_rest = share(0, 1)
    rest = (others - 1, range((pieces - 1) // 2 * 2, pieces))
    lax.fori_loop(1, blocks, tail_row, 0)

    def own_share(n, carry):
        i = n // own_tiles
        at = pl.multiple_of(lax.rem(n, own_tiles) * tile, tile)
        rows = pl.ds(pl.multiple_of(i * BLOCK, BLOCK), BLOCK)

        def put(x):
            kept[rows, pl.ds(at, tile)] = x

        project(i, head, at, tile, put)

        @pl.when(n == 0)
        def _():
            send_rest(blocks - 1, rest if blocks > 1 else first_rest)

        return carry

    lax.fori_loop(0, blocks * own_tiles, own_share, 0)

    for d in range(1, seq_count):
        note_copy(d).wait_send()

    def sent(n, carry):
        kv_copy(n // kv_heads + 1, lax.rem(n, kv_heads)).wait_send()
        return carry

    lax.fori_loop(0, (seq_count - 1) * kv_heads, sent, 0)

    def finish(i, carry):
        rows = pl.ds(pl.multiple_of(i * BLOCK, BLOCK), BLOCK)
        for p in range(pieces):
            total = kept[rows, p * piece : (p + 1) * piece]
            for o in range(others):
                y_copy(o, i, p).wait_recv()
                total = total + yrecv[o, i, p].astype(jnp.float32)
            out_ref[rows, p * piece : (p + 1) * piece] = total.astype(jnp.bfloat16)
            for o in range(others):
                y_copy(o, i, p).wait_send()
        return carry

    lax.fori_loop(0, blocks, finish, 0)


def per_device(queries, keys, values, doc_ids, block_lists, w_out):
    tokens, depth = queries.shape
    blocks = tokens // BLOCK
    kv_width = keys.shape[1]
    kv_heads = kv_width // HEAD_SIZE
    seq_count = lax.axis_size("seq")
    head_count = lax.axis_size("head")
    dp_count = lax.axis_size("dp")
    far = seq_count - 1
    others = head_count - 1
    slots = blocks + far
    cols = w_out.shape[1] // head_count
    pieces = math.gcd(PIECES, cols // LANES)
    note_rows = -(-(blocks + 1) // 8) * 8
    assert DOCS + slots <= LANES
    hbm = pl.BlockSpec(memory_space=pl.ANY)
    bf16, f32, i32 = jnp.bfloat16, jnp.float32, jnp.int32
    half = GROUP // 2 * BLOCK
    return pl.pallas_call(
        functools.partial(kernel, seq_count, head_count, dp_count),
        out_shape=jax.ShapeDtypeStruct((tokens, cols), bf16),
        in_specs=[
            hbm,
        ]
        * 6,
        out_specs=pl.BlockSpec(memory_space=pltpu.VMEM),
        scratch_shapes=[
            pltpu.SMEM(block_lists.shape, i32),
            pltpu.VMEM((blocks, BLOCK), i32),
            pltpu.VMEM((tokens, depth), bf16),
            pltpu.VMEM((tokens, kv_width), bf16),
            pltpu.VMEM((tokens, kv_width), bf16),
            pltpu.VMEM(w_out.shape, bf16),
            pltpu.VMEM((note_rows, LANES), i32),
            pltpu.VMEM((far, note_rows, LANES), i32),
            pltpu.VMEM((far, kv_heads, 2 * BLOCK, HEAD_SIZE), bf16),
            pltpu.VMEM((far, kv_heads, 2 * BLOCK, HEAD_SIZE), bf16),
            pltpu.VMEM((blocks, BLOCK, LANES), bf16),
            pltpu.VMEM((slots * BLOCK, LANES), bf16),
            [pltpu.VMEM((half, max(blocks, far) * BLOCK), f32) for _ in range(2)],
            [pltpu.VMEM((half, max(blocks, far) * BLOCK), bf16) for _ in range(2)],
            pltpu.VMEM((tokens, depth), bf16),
            pltpu.VMEM((others, blocks, pieces, BLOCK, cols // pieces), bf16),
            pltpu.VMEM((others, blocks, pieces, BLOCK, cols // pieces), bf16),
            pltpu.VMEM((tokens, cols), f32),
            pltpu.VMEM((kv_heads * blocks, 2, half, 2 * LANES), f32),
            pltpu.VMEM((kv_heads * blocks, 2, half, LANES), f32),
            pltpu.SemaphoreType.DMA((6,)),
            pltpu.SemaphoreType.DMA((far,)),
            pltpu.SemaphoreType.DMA((far,)),
            pltpu.SemaphoreType.DMA((far, kv_heads)),
            pltpu.SemaphoreType.DMA((far, kv_heads)),
            pltpu.SemaphoreType.DMA((others, blocks, pieces)),
            pltpu.SemaphoreType.DMA((others, blocks, pieces)),
            pltpu.SemaphoreType.REGULAR,
        ],
        compiler_params=pltpu.CompilerParams(
            collective_id=0, has_side_effects=True, vmem_limit_bytes=51500 * 2**10
        ),
    )(
        *[
            pltpu.with_memory_space_constraint(x, pltpu.HBM)
            for x in (
                block_lists,
                doc_ids.reshape(blocks, BLOCK),
                queries,
                keys,
                values,
                w_out,
            )
        ]
    )


def solution(mesh):
    in_specs = (
        P(("dp", "seq"), "head"),
        P(("dp", "seq"), "head"),
        P(("dp", "seq"), "head"),
        P(("dp", "seq")),
        P(("dp", "seq"), None),
        P("head", None),
    )
    out_specs = P(("dp", "seq"), "head")
    return jax.shard_map(
        per_device, mesh=mesh, in_specs=in_specs, out_specs=out_specs, check_vma=False
    )
```

```python
import functools
import math

import jax
import jax.numpy as jnp
from jax import lax
from jax.experimental import pallas as pl
from jax.experimental.pallas import tpu as pltpu
from jax.sharding import PartitionSpec as P

HEAD_SIZE = 128
BLOCK = 128
LANES = 128
DOCS = 8
GROUP = 4
PIECES = 4
TILE = 1024
MESH = pl.DeviceIdType.MESH

far_score = float(2**20)
exp2_scale = math.log2(math.e) / math.sqrt(HEAD_SIZE)


def column_of(row):
    return jnp.broadcast_to(row, (BLOCK, LANES)).astype(jnp.float32).T


def kernel(
    seq_count,
    head_count,
    dp_count,
    lists_hbm,
    docs_hbm,
    q_hbm,
    k_hbm,
    v_hbm,
    w_hbm,
    out_hbm,
    lists_ref,
    docs_ref,
    q_ref,
    k_ref,
    v_ref,
    w_ref,
    note_out,
    note_in,
    stage,
    land,
    qext,
    kext,
    scores,
    probs,
    attn,
    ysend,
    yrecv,
    kept,
    own_sum,
    own_top,
    first_share,
    load_sem,
    note_ssem,
    note_rsem,
    kv_ssem,
    kv_rsem,
    y_ssem,
    y_rsem,
    out_sem,
    turn_sem,
):
    own = lax.axis_index("seq")
    head = lax.axis_index("head")
    core = lax.axis_index("dp")
    blocks = docs_ref.shape[0]
    slots = blocks + seq_count - 1
    kv_heads = k_ref.shape[1] // HEAD_SIZE
    width = GROUP * HEAD_SIZE
    cols = kept.shape[1]
    pieces = ysend.shape[2]
    piece = cols // pieces
    tile = math.gcd(TILE, cols)
    own_tiles = cols // tile
    others = head_count - 1
    last = kv_heads - 1
    middle = 1 + (seq_count - 1) * 4 // 7

    loads = [
        pltpu.make_async_copy(src, dst, load_sem.at[n])
        for n, (src, dst) in enumerate(
            (
                (docs_hbm, docs_ref),
                (lists_hbm, lists_ref),
                (k_hbm, k_ref),
                (v_hbm, v_ref),
                (q_hbm, q_ref),
                (w_hbm, w_ref),
            )
        )
    ]
    for load in loads:
        load.start()

    barrier = pltpu.get_barrier_semaphore()
    for d in range(1, seq_count):
        pl.semaphore_signal(
            barrier, inc=1, device_id={"seq": lax.rem(own + d, seq_count)}, device_id_type=MESH
        )
    for d in range(1, head_count):
        pl.semaphore_signal(
            barrier, inc=1, device_id={"head": lax.rem(head + d, head_count)}, device_id_type=MESH
        )
    for d in range(1, dp_count):
        pl.semaphore_signal(
            barrier, inc=1, device_id={"dp": lax.rem(core + d, dp_count)}, device_id_type=MESH
        )

    loads[0].wait()
    loads[1].wait()

    lane = lax.broadcasted_iota(jnp.int32, (1, LANES), 1)
    slot = lane - DOCS
    source = own - (slot - blocks + 1)
    source = jnp.where(source < 0, source + seq_count, source)
    is_own = (slot >= 0) & (slot < blocks)
    is_far = (slot >= blocks) & (slot < slots)
    low = jnp.where(is_own, own * blocks + slot, jnp.where(is_far, source * blocks, -1))
    high = jnp.where(is_own, low + 1, jnp.where(is_far, low + blocks, -1))
    owner_low = lane * blocks
    asked = jnp.zeros((1, LANES), jnp.int32)
    listed = []
    for i in range(blocks):
        here = jnp.zeros((1, LANES), jnp.int32)
        for j in range(lists_ref.shape[1]):
            block = lists_ref[i, j]
            here = jnp.where((block >= low) & (block < high), 1, here)
            inside = (block >= owner_low) & (block < owner_low + blocks)
            asked = jnp.maximum(asked, jnp.where(inside, block - owner_low + 1, 0))
        listed.append(here)
    for d in range(1, seq_count):
        owner = lax.rem(own + d, seq_count)
        want = jnp.max(jnp.where(lane == owner, asked, 0), axis=1, keepdims=True)
        note_out[d - 1, 0:blocks, :] = docs_ref[...]
        note_out[d - 1, blocks : blocks + 1, :] = jnp.broadcast_to(
            jnp.maximum(want - 1, 0), (1, LANES)
        )

    pl.semaphore_wait(barrier, seq_count + head_count + dp_count - 3)

    def note_copy(d):
        return pltpu.make_async_remote_copy(
            src_ref=note_out.at[d - 1],
            dst_ref=note_in.at[d - 1],
            send_sem=note_ssem,
            recv_sem=note_rsem.at[d - 1],
            device_id={"seq": lax.rem(own + d, seq_count)},
            device_id_type=MESH,
        )

    def kv_copy(d, h):
        return pltpu.make_async_remote_copy(
            src_ref=stage.at[d - 1, h],
            dst_ref=land.at[d - 1, h],
            send_sem=kv_ssem,
            recv_sem=kv_rsem.at[jnp.where((h == last) & (d >= middle), kv_heads, h)],
            device_id={"seq": lax.rem(own + d, seq_count)},
            device_id_type=MESH,
        )

    def other(axis, at, count):
        return {axis: lax.rem(at + 1, count)}

    sides = jnp.minimum(own, seq_count - 1 - own)

    def step_of(n):
        pair = n // 2 + 1
        rest = n - sides + 1
        both = jnp.where(lax.rem(n, 2) == 0, pair, seq_count - pair)
        one = jnp.where(own < seq_count - 1 - own, rest, seq_count - rest)
        return jnp.where(n < 2 * sides, both, one)

    for d in range(1, seq_count):
        note_copy(d).start()
    loads[2].wait()
    loads[3].wait()

    def send_heads(first):
        def send_head(h, carry):
            def send(n, inner):
                kv_copy(n + 1, h).start()
                return inner

            return lax.fori_loop(0, seq_count - 1, send, carry)

        lax.fori_loop(first, kv_heads, send_head, 0)

    lanes = lax.broadcasted_iota(jnp.int32, (BLOCK, LANES), 1)
    lanes_f = lanes.astype(jnp.float32)
    is_doc = lanes < DOCS

    def put_kext(s, row):
        same = jnp.where(column_of(row) == lanes_f, 1.0, 0.0)
        hot = jnp.where(is_doc, same, jnp.where(lanes == DOCS + s, 1.0, 0.0))
        at = s * BLOCK
        if not isinstance(s, int):
            at = pl.multiple_of(at, BLOCK)
        kext[pl.ds(at, BLOCK), :] = hot.astype(jnp.bfloat16)

    for i in range(blocks):
        row = docs_ref[i : i + 1, :]
        put_kext(i, row)
        same = jnp.where(column_of(row) == lanes_f, 0.0, -far_score)
        names = jnp.where(listed[i] > 0, 0.0, -far_score)
        qext[i] = jnp.where(is_doc, same, names).astype(jnp.bfloat16)

    def far_kext():
        for d in range(1, seq_count):
            want = note_out[seq_count - d - 1, blocks : blocks + 1, :]
            note = note_in[d - 1]
            rows = lax.broadcasted_iota(jnp.int32, note.shape, 0)
            row = jnp.max(jnp.where(rows == want, note, 0), axis=0, keepdims=True)
            put_kext(blocks + d - 1, row)

    ones = jnp.ones((BLOCK, LANES), jnp.bfloat16)

    def key_tile(s, h, which):
        if s < blocks:
            ref = v_ref if which else k_ref
            at = h * HEAD_SIZE
            if not isinstance(h, int):
                at = pl.multiple_of(at, HEAD_SIZE)
            return ref[s * BLOCK : (s + 1) * BLOCK, pl.ds(at, HEAD_SIZE)]
        return land[s - blocks, h, which * BLOCK : (which + 1) * BLOCK, :]

    parts = 2
    per = GROUP // parts
    part_rows = per * BLOCK

    def softmax_sums(h, rows, names, put):
        chunks = [names[n : n + 2] for n in range(0, len(names), 2)]
        keys = [
            jnp.concatenate(
                [
                    jnp.concatenate(
                        [key_tile(s, h, 0), kext[s * BLOCK : (s + 1) * BLOCK, :]], axis=1
                    )
                    for s in chunk
                ],
                axis=0,
            )
            for chunk in chunks
        ]
        v = jnp.concatenate(
            [jnp.concatenate([key_tile(s, h, 1), ones], axis=1) for s in names], axis=0
        )
        units = [(i, part) for i in rows for part in range(parts)]

        def score(u):
            i, part = units[u]
            at = pl.multiple_of(i * BLOCK, BLOCK)
            bias = qext[i]
            q = jnp.concatenate(
                [
                    jnp.concatenate(
                        [q_ref[pl.ds(at, BLOCK), head_cols(h, part * per + g)], bias], axis=1
                    )
                    for g in range(per)
                ],
                axis=0,
            )
            top = None
            n = 0
            for k in keys:
                s = lax.dot_general(
                    q, k, (((1,), (1,)), ((), ())), preferred_element_type=jnp.float32
                )
                for m in range(k.shape[0] // BLOCK):
                    t = s[:, m * BLOCK : (m + 1) * BLOCK]
                    scores[u % 2][:, n * BLOCK : (n + 1) * BLOCK] = t
                    top = t if top is None else jnp.maximum(top, t)
                    n += 1
            return top

        top = score(0)
        for u, (i, part) in enumerate(units):
            later = score(u + 1) if u + 1 < len(units) else None
            top = jnp.max(top, axis=1, keepdims=True)
            for n in range(len(names)):
                here = slice(n * BLOCK, (n + 1) * BLOCK)
                probs[u % 2][:, here] = jnp.exp2(
                    (scores[u % 2][:, here] - top) * exp2_scale
                ).astype(jnp.bfloat16)
            o = jnp.dot(
                probs[u % 2][:, : len(names) * BLOCK], v, preferred_element_type=jnp.float32
            )
            put(i, part, top, o)
            top = later

    def head_cols(h, g):
        return pl.ds(pl.multiple_of(h * width + g * HEAD_SIZE, HEAD_SIZE), HEAD_SIZE)

    own_slots = list(range(blocks))
    far_slots = list(range(blocks, slots))

    span = math.gcd(blocks, 2)
    steps = blocks // span

    def rows_of(n):
        return [n * span + r for r in range(span)]

    def attend_own(n, carry):
        h = n // steps

        def put(i, part, top, o):
            own_top[h * blocks + i, part] = jnp.broadcast_to(top, (part_rows, LANES))
            own_sum[h * blocks + i, part] = o

        softmax_sums(h, rows_of(lax.rem(n, steps)), own_slots, put)
        return carry

    def attend(h, rows, names=far_slots, final=True):
        def put(i, part, top, o):
            at = pl.multiple_of(i * BLOCK, BLOCK)
            n = h * blocks + i
            first = own_top[n, part]
            both = jnp.maximum(first, top)
            near = jnp.exp2((first - both) * exp2_scale)
            far = jnp.exp2((top - both) * exp2_scale)
            x = own_sum[n, part]
            total = x[:, :HEAD_SIZE] * near + o[:, :HEAD_SIZE] * far
            count = x[:, HEAD_SIZE:] * near + o[:, HEAD_SIZE:] * far
            if not final:
                own_top[n, part] = both
                own_sum[n, part, :, :HEAD_SIZE] = total
                own_sum[n, part, :, HEAD_SIZE:] = count
                return
            result = (total / count).astype(jnp.bfloat16)
            for g in range(per):
                attn[pl.ds(at, BLOCK), head_cols(h, part * per + g)] = result[
                    g * BLOCK : (g + 1) * BLOCK
                ]

        softmax_sums(h, rows, names, put)

    def pick(d, heads):
        want = note_in[seq_count - d - 1, blocks : blocks + 1, :]
        want = jnp.broadcast_to(want, (BLOCK, LANES))
        hots = [jnp.where(want == b, 1.0, 0.0).astype(jnp.bfloat16) for b in range(blocks)]
        for h in heads:
            cut = slice(h * HEAD_SIZE, (h + 1) * HEAD_SIZE)
            for part, ref in enumerate((k_ref, v_ref)):
                picked = None
                for b in range(blocks):
                    term = ref[b * BLOCK : (b + 1) * BLOCK, cut] * hots[b]
                    picked = term if picked is None else picked + term
                stage[d - 1, h, part * BLOCK : (part + 1) * BLOCK, :] = picked

    def fill_first(n, carry):
        d = step_of(n)
        note_copy(seq_count - d).wait_recv()
        pick(d, [0])

        @pl.when((core == 0) & (n > 0))
        def _():
            kv_copy(step_of(n - 1), 0).start()

        return carry

    def fill_rest(n, carry):
        pick(step_of(n), range(1, kv_heads))
        return carry

    own_steps = kv_heads * steps
    lax.fori_loop(0, seq_count - 1, fill_first, 0)
    lax.fori_loop(0, 1, fill_rest, 0)

    @pl.when(core == 0)
    def _():
        kv_copy(step_of(seq_count - 2), 0).start()

    lax.fori_loop(1, seq_count - 1, fill_rest, 0)

    @pl.when(core == 0)
    def _():
        send_heads(1)

    loads[4].wait()
    lax.fori_loop(0, own_steps, attend_own, 0)

    @pl.when(core > 0)
    def _():
        pl.semaphore_wait(turn_sem, 1)
        send_heads(0)

    far_kext()

    def wait_blocks(h, first, end, sem):
        part = pl.ds(first - 1, end - first)
        pltpu.make_async_remote_copy(
            src_ref=stage.at[part, h],
            dst_ref=land.at[part, h],
            send_sem=kv_ssem,
            recv_sem=kv_rsem.at[sem],
            device_id=other("seq", own, seq_count),
            device_id_type=MESH,
        ).wait_recv()

    def wait_head(h):
        wait_blocks(h, 1, seq_count, h)

    def one_head(h, carry):
        wait_head(h)

        def one_row(i, inner):
            attend(h, rows_of(i))
            return inner

        return lax.fori_loop(0, steps, one_row, carry)

    before_last = max(last - 1, 0)
    lax.fori_loop(0, before_last, one_head, 0)
    for h in range(before_last, last):
        wait_head(h)
        attend(h, [0])

    @pl.when(core + 1 < dp_count)
    def _():
        pl.semaphore_signal(turn_sem, inc=1, device_id={"dp": core + 1}, device_id_type=MESH)

    loads[5].wait()

    early = last * width
    if early:
        for o in range(others):
            target = lax.rem(head + o + 1, head_count)
            for at in range(0, cols, piece):
                start = pl.multiple_of(target * cols + at, piece)
                first_share[o, :, at : at + piece] = jnp.dot(
                    attn[0:BLOCK, :early],
                    w_ref[:early, pl.ds(start, piece)],
                    preferred_element_type=jnp.float32,
                )

    wait_blocks(last, 1, middle, last)
    attend(last, [0], far_slots[: middle - 1], False)
    wait_blocks(last, middle, seq_count, kv_heads)

    def project(i, target, at, size, put):
        rows = attn[pl.ds(pl.multiple_of(i * BLOCK, BLOCK), BLOCK), :]
        start = pl.multiple_of(target * cols + at, size)
        put(jnp.dot(rows, w_ref[:, pl.ds(start, size)], preferred_element_type=jnp.float32))

    def y_copy(o, i, p):
        return pltpu.make_async_remote_copy(
            src_ref=ysend.at[o, i, p],
            dst_ref=yrecv.at[o, i, p],
            send_sem=y_ssem,
            recv_sem=y_rsem.at[o, jnp.where(i < blocks - 1, i, blocks - 1 + p)],
            device_id={"head": lax.rem(head + o + 1, head_count)},
            device_id_type=MESH,
        )

    def share(i, size):
        groups = [
            (o, range(p, min(p + size, pieces)))
            for o in range(others)
            for p in range(0, pieces, size)
        ]
        for n, (o, group) in enumerate(groups):
            target = lax.rem(head + o + 1, head_count)

            def put(x):
                for p in group:
                    at = (p - group[0]) * piece
                    ysend[o, i, p] = x[:, at : at + piece].astype(jnp.bfloat16)

            if isinstance(i, int) and early:
                at = group[0] * piece
                size_here = len(group) * piece
                start = pl.multiple_of(target * cols + at, size_here)
                put(
                    first_share[o, :, at : at + size_here]
                    + jnp.dot(
                        attn[0:BLOCK, early:],
                        w_ref[early:, pl.ds(start, size_here)],
                        preferred_element_type=jnp.float32,
                    )
                )
            else:
                project(i, target, group[0] * piece, len(group) * piece, put)
            if n > 0:
                for p in groups[n - 1][1]:
                    y_copy(groups[n - 1][0], i, p).start()
        return groups[-1]

    def send_rest(i, group):
        for p in group[1]:
            y_copy(group[0], i, p).start()

    def tail_row(i, carry):
        for h in range(before_last, last):
            attend(h, [i])

        @pl.when(i == 1)
        def _():
            send_rest(0, first_rest)

        @pl.when(i > 1)
        def _():
            send_rest(i - 1, rest)

        attend(last, [i])
        share(i, 2)
        return carry

    attend(last, [0], far_slots[middle - 1 :])
    first_rest = share(0, 1)
    rest = (others - 1, range((pieces - 1) // 2 * 2, pieces))
    lax.fori_loop(1, blocks, tail_row, 0)

    def own_share(n, carry):
        i = n // own_tiles
        at = pl.multiple_of(lax.rem(n, own_tiles) * tile, tile)
        rows = pl.ds(pl.multiple_of(i * BLOCK, BLOCK), BLOCK)

        def put(x):
            kept[rows, pl.ds(at, tile)] = x.astype(jnp.bfloat16)

        project(i, head, at, tile, put)

        @pl.when(n == 0)
        def _():
            send_rest(blocks - 1, rest if blocks > 1 else first_rest)

        return carry

    lax.fori_loop(0, blocks * own_tiles, own_share, 0)

    def all_sent(src, dst, sem, unused, axis, at, count):
        pltpu.make_async_remote_copy(
            src_ref=src,
            dst_ref=dst,
            send_sem=sem,
            recv_sem=unused,
            device_id=other(axis, at, count),
            device_id_type=MESH,
        ).wait_send()

    all_sent(note_out, note_in, note_ssem, note_rsem.at[0], "seq", own, seq_count)
    all_sent(stage, land, kv_ssem, kv_rsem.at[0], "seq", own, seq_count)

    def out_copy(rows, part):
        return pltpu.make_async_copy(kept.at[rows, part], out_hbm.at[rows, part], out_sem)

    def add(rows, i, p):
        part = slice(p * piece, (p + 1) * piece)
        total = kept[rows, part].astype(jnp.float32)
        for o in range(others):
            total = total + yrecv[o, i, p].astype(jnp.float32)
        kept[rows, part] = total.astype(jnp.bfloat16)
        out_copy(rows, pl.ds(p * piece, piece)).start()

    def finish(i, carry):
        for o in range(others):
            pltpu.make_async_remote_copy(
                src_ref=ysend.at[o, i],
                dst_ref=yrecv.at[o, i],
                send_sem=y_ssem,
                recv_sem=y_rsem.at[o, i],
                device_id=other("head", head, head_count),
                device_id_type=MESH,
            ).wait_recv()
        for p in range(pieces):
            add(pl.ds(pl.multiple_of(i * BLOCK, BLOCK), BLOCK), i, p)
        return carry

    lax.fori_loop(0, blocks - 1, finish, 0)
    for p in range(pieces):
        for o in range(others):
            y_copy(o, blocks - 1, p).wait_recv()
        add(pl.ds((blocks - 1) * BLOCK, BLOCK), blocks - 1, p)

    all_sent(ysend, yrecv, y_ssem, y_rsem.at[0, 0], "head", head, head_count)
    pltpu.make_async_copy(kept, out_hbm, out_sem).wait()


def per_device(queries, keys, values, doc_ids, block_lists, w_out):
    tokens, depth = queries.shape
    blocks = tokens // BLOCK
    kv_width = keys.shape[1]
    kv_heads = kv_width // HEAD_SIZE
    seq_count = lax.axis_size("seq")
    head_count = lax.axis_size("head")
    dp_count = lax.axis_size("dp")
    far = seq_count - 1
    others = head_count - 1
    slots = blocks + far
    cols = w_out.shape[1] // head_count
    pieces = math.gcd(PIECES, cols // LANES)
    note_rows = -(-(blocks + 1) // 8) * 8
    assert DOCS + slots <= LANES
    hbm = pl.BlockSpec(memory_space=pl.ANY)
    bf16, f32, i32 = jnp.bfloat16, jnp.float32, jnp.int32
    half = GROUP // 2 * BLOCK
    return pl.pallas_call(
        functools.partial(kernel, seq_count, head_count, dp_count),
        out_shape=jax.ShapeDtypeStruct((tokens, cols), bf16),
        in_specs=[
            hbm,
        ]
        * 6,
        out_specs=hbm,
        scratch_shapes=[
            pltpu.SMEM(block_lists.shape, i32),
            pltpu.VMEM((blocks, BLOCK), i32),
            pltpu.VMEM((tokens, depth), bf16),
            pltpu.VMEM((tokens, kv_width), bf16),
            pltpu.VMEM((tokens, kv_width), bf16),
            pltpu.VMEM(w_out.shape, bf16),
            pltpu.VMEM((far, note_rows, LANES), i32),
            pltpu.VMEM((far, note_rows, LANES), i32),
            pltpu.VMEM((far, kv_heads, 2 * BLOCK, HEAD_SIZE), bf16),
            pltpu.VMEM((far, kv_heads, 2 * BLOCK, HEAD_SIZE), bf16),
            pltpu.VMEM((blocks, BLOCK, LANES), bf16),
            pltpu.VMEM((slots * BLOCK, LANES), bf16),
            [pltpu.VMEM((half, max(blocks, far) * BLOCK), f32) for _ in range(2)],
            [pltpu.VMEM((half, max(blocks, far) * BLOCK), bf16) for _ in range(2)],
            pltpu.VMEM((tokens, depth), bf16),
            pltpu.VMEM((others, blocks, pieces, BLOCK, cols // pieces), bf16),
            pltpu.VMEM((others, blocks, pieces, BLOCK, cols // pieces), bf16),
            pltpu.VMEM((tokens, cols), bf16),
            pltpu.VMEM((kv_heads * blocks, 2, half, 2 * LANES), f32),
            pltpu.VMEM((kv_heads * blocks, 2, half, LANES), f32),
            pltpu.VMEM((others, BLOCK, cols), f32),
            pltpu.SemaphoreType.DMA((6,)),
            pltpu.SemaphoreType.DMA,
            pltpu.SemaphoreType.DMA((far,)),
            pltpu.SemaphoreType.DMA,
            pltpu.SemaphoreType.DMA((kv_heads + 1,)),
            pltpu.SemaphoreType.DMA,
            pltpu.SemaphoreType.DMA((others, blocks - 1 + pieces)),
            pltpu.SemaphoreType.DMA,
            pltpu.SemaphoreType.REGULAR,
        ],
        compiler_params=pltpu.CompilerParams(
            collective_id=0, has_side_effects=True, vmem_limit_bytes=51500 * 2**10
        ),
    )(
        *[
            pltpu.with_memory_space_constraint(x, pltpu.HBM)
            for x in (
                block_lists,
                doc_ids.reshape(blocks, BLOCK),
                queries,
                keys,
                values,
                w_out,
            )
        ]
    )


def solution(mesh):
    in_specs = (
        P(("dp", "seq"), "head"),
        P(("dp", "seq"), "head"),
        P(("dp", "seq"), "head"),
        P(("dp", "seq")),
        P(("dp", "seq"), None),
        P("head", None),
    )
    out_specs = P(("dp", "seq"), "head")
    return jax.shard_map(
        per_device, mesh=mesh, in_specs=in_specs, out_specs=out_specs, check_vma=False
    )
```

```python
import functools
import math

import jax
import jax.numpy as jnp
from jax import lax
from jax.experimental import pallas as pl
from jax.experimental.pallas import tpu as pltpu
from jax.sharding import PartitionSpec as P

HEAD_SIZE = 128
BLOCK = 128
LANES = 128
DOCS = 8
GROUP = 4
PIECES = 4
TILE = 1024
MESH = pl.DeviceIdType.MESH

far_score = float(2**20)
exp2_scale = math.log2(math.e) / math.sqrt(HEAD_SIZE)


def column_of(row):
    return jnp.broadcast_to(row, (BLOCK, LANES)).astype(jnp.float32).T


def kernel(
    seq_count,
    head_count,
    dp_count,
    lists_hbm,
    docs_hbm,
    q_hbm,
    k_hbm,
    v_hbm,
    w_hbm,
    out_hbm,
    lists_ref,
    docs_ref,
    q_ref,
    k_ref,
    v_ref,
    w_ref,
    note_out,
    note_in,
    stage,
    land,
    qext,
    kext,
    scores,
    probs,
    attn,
    ysend,
    yrecv,
    kept,
    own_sum,
    own_top,
    first_share,
    load_sem,
    note_ssem,
    note_rsem,
    kv_ssem,
    kv_rsem,
    y_ssem,
    y_rsem,
    out_sem,
    turn_sem,
):
    own = lax.axis_index("seq")
    head = lax.axis_index("head")
    core = lax.axis_index("dp")
    blocks = docs_ref.shape[0]
    slots = blocks + seq_count - 1
    kv_heads = k_ref.shape[1] // HEAD_SIZE
    width = GROUP * HEAD_SIZE
    cols = kept.shape[1]
    pieces = ysend.shape[2]
    piece = cols // pieces
    tile = math.gcd(TILE, cols)
    own_tiles = cols // tile
    others = head_count - 1
    last = kv_heads - 1
    middle = 1 + (seq_count - 1) * 4 // 7

    loads = [
        pltpu.make_async_copy(src, dst, load_sem.at[n])
        for n, (src, dst) in enumerate(
            (
                (docs_hbm, docs_ref),
                (lists_hbm, lists_ref),
                (k_hbm, k_ref),
                (v_hbm, v_ref),
                (q_hbm, q_ref),
                (w_hbm, w_ref),
            )
        )
    ]
    for load in loads:
        load.start()

    barrier = pltpu.get_barrier_semaphore()
    for d in range(1, seq_count):
        pl.semaphore_signal(
            barrier, inc=1, device_id={"seq": lax.rem(own + d, seq_count)}, device_id_type=MESH
        )
    for d in range(1, head_count):
        pl.semaphore_signal(
            barrier, inc=1, device_id={"head": lax.rem(head + d, head_count)}, device_id_type=MESH
        )
    for d in range(1, dp_count):
        pl.semaphore_signal(
            barrier, inc=1, device_id={"dp": lax.rem(core + d, dp_count)}, device_id_type=MESH
        )

    loads[0].wait()
    loads[1].wait()

    lane = lax.broadcasted_iota(jnp.int32, (1, LANES), 1)
    slot = lane - DOCS
    source = own - (slot - blocks + 1)
    source = jnp.where(source < 0, source + seq_count, source)
    is_own = (slot >= 0) & (slot < blocks)
    is_far = (slot >= blocks) & (slot < slots)
    low = jnp.where(is_own, own * blocks + slot, jnp.where(is_far, source * blocks, -1))
    high = jnp.where(is_own, low + 1, jnp.where(is_far, low + blocks, -1))
    owner_low = lane * blocks
    asked = jnp.zeros((1, LANES), jnp.int32)
    listed = []
    for i in range(blocks):
        here = jnp.zeros((1, LANES), jnp.int32)
        for j in range(lists_ref.shape[1]):
            block = lists_ref[i, j]
            here = jnp.where((block >= low) & (block < high), 1, here)
            inside = (block >= owner_low) & (block < owner_low + blocks)
            asked = jnp.maximum(asked, jnp.where(inside, block - owner_low + 1, 0))
        listed.append(here)
    for d in range(1, seq_count):
        owner = lax.rem(own + d, seq_count)
        want = jnp.max(jnp.where(lane == owner, asked, 0), axis=1, keepdims=True)
        note_out[d - 1, 0:blocks, :] = docs_ref[...]
        note_out[d - 1, blocks : blocks + 1, :] = jnp.broadcast_to(
            jnp.maximum(want - 1, 0), (1, LANES)
        )

    pl.semaphore_wait(barrier, seq_count + head_count + dp_count - 3)

    def note_copy(d):
        return pltpu.make_async_remote_copy(
            src_ref=note_out.at[d - 1],
            dst_ref=note_in.at[d - 1],
            send_sem=note_ssem,
            recv_sem=note_rsem.at[d - 1],
            device_id={"seq": lax.rem(own + d, seq_count)},
            device_id_type=MESH,
        )

    def kv_copy(d, h):
        return pltpu.make_async_remote_copy(
            src_ref=stage.at[d - 1, h],
            dst_ref=land.at[d - 1, h],
            send_sem=kv_ssem,
            recv_sem=kv_rsem.at[jnp.where((h == last) & (d >= middle), kv_heads, h)],
            device_id={"seq": lax.rem(own + d, seq_count)},
            device_id_type=MESH,
        )

    def other(axis, at, count):
        return {axis: lax.rem(at + 1, count)}

    sides = jnp.minimum(own, seq_count - 1 - own)

    def step_of(n):
        pair = n // 2 + 1
        rest = n - sides + 1
        both = jnp.where(lax.rem(n, 2) == 0, pair, seq_count - pair)
        one = jnp.where(own < seq_count - 1 - own, rest, seq_count - rest)
        return jnp.where(n < 2 * sides, both, one)

    for d in range(1, seq_count):
        note_copy(d).start()
    loads[2].wait()
    loads[3].wait()

    def send_heads(first):
        def send_head(h, carry):
            def send(n, inner):
                d = jnp.where(core == 0, n + 1, step_of(seq_count - 2 - n))
                kv_copy(d, h).start()
                return inner

            return lax.fori_loop(0, seq_count - 1, send, carry)

        lax.fori_loop(first, kv_heads, send_head, 0)

    lanes = lax.broadcasted_iota(jnp.int32, (BLOCK, LANES), 1)
    lanes_f = lanes.astype(jnp.float32)
    is_doc = lanes < DOCS

    def put_kext(s, row):
        same = jnp.where(column_of(row) == lanes_f, 1.0, 0.0)
        hot = jnp.where(is_doc, same, jnp.where(lanes == DOCS + s, 1.0, 0.0))
        at = s * BLOCK
        if not isinstance(s, int):
            at = pl.multiple_of(at, BLOCK)
        kext[pl.ds(at, BLOCK), :] = hot.astype(jnp.bfloat16)

    for i in range(blocks):
        row = docs_ref[i : i + 1, :]
        put_kext(i, row)
        same = jnp.where(column_of(row) == lanes_f, 0.0, -far_score)
        names = jnp.where(listed[i] > 0, 0.0, -far_score)
        qext[i] = jnp.where(is_doc, same, names).astype(jnp.bfloat16)

    def far_kext():
        for d in range(1, seq_count):
            want = note_out[seq_count - d - 1, blocks : blocks + 1, :]
            note = note_in[d - 1]
            rows = lax.broadcasted_iota(jnp.int32, note.shape, 0)
            row = jnp.max(jnp.where(rows == want, note, 0), axis=0, keepdims=True)
            put_kext(blocks + d - 1, row)

    ones = jnp.ones((BLOCK, LANES), jnp.bfloat16)

    def key_tile(s, h, which):
        if s < blocks:
            ref = v_ref if which else k_ref
            at = h * HEAD_SIZE
            if not isinstance(h, int):
                at = pl.multiple_of(at, HEAD_SIZE)
            return ref[s * BLOCK : (s + 1) * BLOCK, pl.ds(at, HEAD_SIZE)]
        return land[s - blocks, h, which * BLOCK : (which + 1) * BLOCK, :]

    parts = 2
    per = GROUP // parts
    part_rows = per * BLOCK

    def softmax_sums(h, rows, names, put):
        chunks = [names[n : n + 2] for n in range(0, len(names), 2)]
        keys = [
            jnp.concatenate(
                [
                    jnp.concatenate(
                        [key_tile(s, h, 0), kext[s * BLOCK : (s + 1) * BLOCK, :]], axis=1
                    )
                    for s in chunk
                ],
                axis=0,
            )
            for chunk in chunks
        ]
        v = jnp.concatenate(
            [jnp.concatenate([key_tile(s, h, 1), ones], axis=1) for s in names], axis=0
        )
        units = [(i, part) for i in rows for part in range(parts)]

        def score(u):
            i, part = units[u]
            at = pl.multiple_of(i * BLOCK, BLOCK)
            bias = qext[i]
            q = jnp.concatenate(
                [
                    jnp.concatenate(
                        [q_ref[pl.ds(at, BLOCK), head_cols(h, part * per + g)], bias], axis=1
                    )
                    for g in range(per)
                ],
                axis=0,
            )
            top = None
            n = 0
            for k in keys:
                s = lax.dot_general(
                    q, k, (((1,), (1,)), ((), ())), preferred_element_type=jnp.float32
                )
                for m in range(k.shape[0] // BLOCK):
                    t = s[:, m * BLOCK : (m + 1) * BLOCK]
                    scores[u % 2][:, n * BLOCK : (n + 1) * BLOCK] = t
                    top = t if top is None else jnp.maximum(top, t)
                    n += 1
            return top

        top = score(0)
        for u, (i, part) in enumerate(units):
            later = score(u + 1) if u + 1 < len(units) else None
            top = jnp.max(top, axis=1, keepdims=True)
            for n in range(len(names)):
                here = slice(n * BLOCK, (n + 1) * BLOCK)
                probs[u % 2][:, here] = jnp.exp2(
                    (scores[u % 2][:, here] - top) * exp2_scale
                ).astype(jnp.bfloat16)
            o = jnp.dot(
                probs[u % 2][:, : len(names) * BLOCK], v, preferred_element_type=jnp.float32
            )
            put(i, part, top, o)
            top = later

    def head_cols(h, g):
        return pl.ds(pl.multiple_of(h * width + g * HEAD_SIZE, HEAD_SIZE), HEAD_SIZE)

    own_slots = list(range(blocks))
    far_slots = list(range(blocks, slots))

    span = math.gcd(blocks, 2)
    steps = blocks // span

    def rows_of(n):
        return [n * span + r for r in range(span)]

    def attend_own(n, carry):
        h = n // steps

        def put(i, part, top, o):
            own_top[h * blocks + i, part] = jnp.broadcast_to(top, (part_rows, LANES))
            own_sum[h * blocks + i, part] = o

        softmax_sums(h, rows_of(lax.rem(n, steps)), own_slots, put)
        return carry

    def attend(h, rows, names=far_slots, final=True):
        def put(i, part, top, o):
            at = pl.multiple_of(i * BLOCK, BLOCK)
            n = h * blocks + i
            first = own_top[n, part]
            both = jnp.maximum(first, top)
            near = jnp.exp2((first - both) * exp2_scale)
            far = jnp.exp2((top - both) * exp2_scale)
            x = own_sum[n, part]
            total = x[:, :HEAD_SIZE] * near + o[:, :HEAD_SIZE] * far
            count = x[:, HEAD_SIZE:] * near + o[:, HEAD_SIZE:] * far
            if not final:
                own_top[n, part] = both
                own_sum[n, part, :, :HEAD_SIZE] = total
                own_sum[n, part, :, HEAD_SIZE:] = count
                return
            result = (total / count).astype(jnp.bfloat16)
            for g in range(per):
                attn[pl.ds(at, BLOCK), head_cols(h, part * per + g)] = result[
                    g * BLOCK : (g + 1) * BLOCK
                ]

        softmax_sums(h, rows, names, put)

    def pick(d, heads):
        want = note_in[seq_count - d - 1, blocks : blocks + 1, :]
        want = jnp.broadcast_to(want, (BLOCK, LANES))
        hots = [jnp.where(want == b, 1.0, 0.0).astype(jnp.bfloat16) for b in range(blocks)]
        for h in heads:
            cut = slice(h * HEAD_SIZE, (h + 1) * HEAD_SIZE)
            for part, ref in enumerate((k_ref, v_ref)):
                picked = None
                for b in range(blocks):
                    term = ref[b * BLOCK : (b + 1) * BLOCK, cut] * hots[b]
                    picked = term if picked is None else picked + term
                stage[d - 1, h, part * BLOCK : (part + 1) * BLOCK, :] = picked

    def fill_first(n, carry):
        d = step_of(n)
        note_copy(seq_count - d).wait_recv()
        pick(d, [0])

        @pl.when((core == 0) & (n > 0))
        def _():
            kv_copy(step_of(n - 1), 0).start()

        return carry

    def fill_rest(n, carry):
        pick(step_of(n), range(1, kv_heads))
        return carry

    own_steps = kv_heads * steps
    lax.fori_loop(0, seq_count - 1, fill_first, 0)
    lax.fori_loop(0, 1, fill_rest, 0)

    @pl.when(core == 0)
    def _():
        kv_copy(step_of(seq_count - 2), 0).start()

    lax.fori_loop(1, seq_count - 1, fill_rest, 0)

    @pl.when(core == 0)
    def _():
        send_heads(1)

    loads[4].wait()
    lax.fori_loop(0, own_steps, attend_own, 0)

    @pl.when(core > 0)
    def _():
        pl.semaphore_wait(turn_sem, 1)
        send_heads(0)

    far_kext()

    def wait_blocks(h, first, end, sem):
        part = pl.ds(first - 1, end - first)
        pltpu.make_async_remote_copy(
            src_ref=stage.at[part, h],
            dst_ref=land.at[part, h],
            send_sem=kv_ssem,
            recv_sem=kv_rsem.at[sem],
            device_id=other("seq", own, seq_count),
            device_id_type=MESH,
        ).wait_recv()

    def wait_head(h):
        wait_blocks(h, 1, seq_count, h)

    def one_head(h, carry):
        wait_head(h)

        def one_row(i, inner):
            attend(h, rows_of(i))
            return inner

        return lax.fori_loop(0, steps, one_row, carry)

    before_last = max(last - 1, 0)
    lax.fori_loop(0, before_last, one_head, 0)
    for h in range(before_last, last):
        wait_head(h)
        attend(h, [0])

    @pl.when(core + 1 < dp_count)
    def _():
        pl.semaphore_signal(turn_sem, inc=1, device_id={"dp": core + 1}, device_id_type=MESH)

    loads[5].wait()

    early = last * width
    if early:
        for o in range(others):
            target = lax.rem(head + o + 1, head_count)
            for at in range(0, cols, piece):
                start = pl.multiple_of(target * cols + at, piece)
                first_share[o, :, at : at + piece] = jnp.dot(
                    attn[0:BLOCK, :early],
                    w_ref[:early, pl.ds(start, piece)],
                    preferred_element_type=jnp.float32,
                )

    wait_blocks(last, 1, middle, last)
    attend(last, [0], far_slots[: middle - 1], False)
    wait_blocks(last, middle, seq_count, kv_heads)

    def project(i, target, at, size, put):
        rows = attn[pl.ds(pl.multiple_of(i * BLOCK, BLOCK), BLOCK), :]
        start = pl.multiple_of(target * cols + at, size)
        put(jnp.dot(rows, w_ref[:, pl.ds(start, size)], preferred_element_type=jnp.float32))

    def y_copy(o, i, p):
        return pltpu.make_async_remote_copy(
            src_ref=ysend.at[o, i, p],
            dst_ref=yrecv.at[o, i, p],
            send_sem=y_ssem,
            recv_sem=y_rsem.at[o, jnp.where(i < blocks - 1, i, blocks - 1 + p)],
            device_id={"head": lax.rem(head + o + 1, head_count)},
            device_id_type=MESH,
        )

    def share(i, size):
        groups = [
            (o, range(p, min(p + size, pieces)))
            for o in range(others)
            for p in range(0, pieces, size)
        ]
        for n, (o, group) in enumerate(groups):
            target = lax.rem(head + o + 1, head_count)

            def put(x):
                for p in group:
                    at = (p - group[0]) * piece
                    ysend[o, i, p] = x[:, at : at + piece].astype(jnp.bfloat16)

            if isinstance(i, int) and early:
                at = group[0] * piece
                size_here = len(group) * piece
                start = pl.multiple_of(target * cols + at, size_here)
                put(
                    first_share[o, :, at : at + size_here]
                    + jnp.dot(
                        attn[0:BLOCK, early:],
                        w_ref[early:, pl.ds(start, size_here)],
                        preferred_element_type=jnp.float32,
                    )
                )
            else:
                project(i, target, group[0] * piece, len(group) * piece, put)
            if n > 0:
                for p in groups[n - 1][1]:
                    y_copy(groups[n - 1][0], i, p).start()
        return groups[-1]

    def send_rest(i, group):
        for p in group[1]:
            y_copy(group[0], i, p).start()

    def tail_row(i, carry):
        for h in range(before_last, last):
            attend(h, [i])

        @pl.when(i == 1)
        def _():
            send_rest(0, first_rest)

        @pl.when(i > 1)
        def _():
            send_rest(i - 1, rest)

        attend(last, [i])
        share(i, 2)
        return carry

    attend(last, [0], far_slots[middle - 1 :])
    first_rest = share(0, 1)
    rest = (others - 1, range((pieces - 1) // 2 * 2, pieces))
    lax.fori_loop(1, blocks, tail_row, 0)

    def own_share(n, carry):
        i = n // own_tiles
        at = pl.multiple_of(lax.rem(n, own_tiles) * tile, tile)
        rows = pl.ds(pl.multiple_of(i * BLOCK, BLOCK), BLOCK)

        def put(x):
            kept[rows, pl.ds(at, tile)] = x.astype(jnp.bfloat16)

        project(i, head, at, tile, put)

        @pl.when(n == 0)
        def _():
            send_rest(blocks - 1, rest if blocks > 1 else first_rest)

        return carry

    lax.fori_loop(0, blocks * own_tiles, own_share, 0)

    def all_sent(src, dst, sem, unused, axis, at, count):
        pltpu.make_async_remote_copy(
            src_ref=src,
            dst_ref=dst,
            send_sem=sem,
            recv_sem=unused,
            device_id=other(axis, at, count),
            device_id_type=MESH,
        ).wait_send()

    all_sent(note_out, note_in, note_ssem, note_rsem.at[0], "seq", own, seq_count)
    all_sent(stage, land, kv_ssem, kv_rsem.at[0], "seq", own, seq_count)

    def block_rows(i):
        return pl.ds(pl.multiple_of(i * BLOCK, BLOCK), BLOCK)

    def out_copy(i, part):
        rows = block_rows(i)
        return pltpu.make_async_copy(kept.at[rows, part], out_hbm.at[rows, part], out_sem)

    def add(i, p):
        rows, part = block_rows(i), slice(p * piece, (p + 1) * piece)
        total = kept[rows, part].astype(jnp.float32)
        for o in range(others):
            total = total + yrecv[o, i, p].astype(jnp.float32)
        kept[rows, part] = total.astype(jnp.bfloat16)

    def finish(i, carry):
        for o in range(others):
            pltpu.make_async_remote_copy(
                src_ref=ysend.at[o, i],
                dst_ref=yrecv.at[o, i],
                send_sem=y_ssem,
                recv_sem=y_rsem.at[o, i],
                device_id=other("head", head, head_count),
                device_id_type=MESH,
            ).wait_recv()
        for p in range(pieces):
            add(i, p)

        @pl.when(i > 0)
        def _():
            out_copy(i - 1, pl.ds(0, cols)).start()

        return carry

    end = blocks - 1
    lax.fori_loop(0, end, finish, 0)
    for p in range(pieces):
        for o in range(others):
            y_copy(o, end, p).wait_recv()
        add(end, p)
        if p > 0:
            out_copy(end, pl.ds((p - 1) * piece, piece)).start()
        elif end > 0:
            out_copy(end - 1, pl.ds(0, cols)).start()

    all_sent(ysend, yrecv, y_ssem, y_rsem.at[0, 0], "head", head, head_count)
    out_copy(end, pl.ds((pieces - 1) * piece, piece)).start()
    pltpu.make_async_copy(kept, out_hbm, out_sem).wait()


def per_device(queries, keys, values, doc_ids, block_lists, w_out):
    tokens, depth = queries.shape
    blocks = tokens // BLOCK
    kv_width = keys.shape[1]
    kv_heads = kv_width // HEAD_SIZE
    seq_count = lax.axis_size("seq")
    head_count = lax.axis_size("head")
    dp_count = lax.axis_size("dp")
    far = seq_count - 1
    others = head_count - 1
    slots = blocks + far
    cols = w_out.shape[1] // head_count
    pieces = math.gcd(PIECES, cols // LANES)
    note_rows = -(-(blocks + 1) // 8) * 8
    assert DOCS + slots <= LANES
    hbm = pl.BlockSpec(memory_space=pl.ANY)
    bf16, f32, i32 = jnp.bfloat16, jnp.float32, jnp.int32
    half = GROUP // 2 * BLOCK
    return pl.pallas_call(
        functools.partial(kernel, seq_count, head_count, dp_count),
        out_shape=jax.ShapeDtypeStruct((tokens, cols), bf16),
        in_specs=[
            hbm,
        ]
        * 6,
        out_specs=hbm,
        scratch_shapes=[
            pltpu.SMEM(block_lists.shape, i32),
            pltpu.VMEM((blocks, BLOCK), i32),
            pltpu.VMEM((tokens, depth), bf16),
            pltpu.VMEM((tokens, kv_width), bf16),
            pltpu.VMEM((tokens, kv_width), bf16),
            pltpu.VMEM(w_out.shape, bf16),
            pltpu.VMEM((far, note_rows, LANES), i32),
            pltpu.VMEM((far, note_rows, LANES), i32),
            pltpu.VMEM((far, kv_heads, 2 * BLOCK, HEAD_SIZE), bf16),
            pltpu.VMEM((far, kv_heads, 2 * BLOCK, HEAD_SIZE), bf16),
            pltpu.VMEM((blocks, BLOCK, LANES), bf16),
            pltpu.VMEM((slots * BLOCK, LANES), bf16),
            [pltpu.VMEM((half, max(blocks, far) * BLOCK), f32) for _ in range(2)],
            [pltpu.VMEM((half, max(blocks, far) * BLOCK), bf16) for _ in range(2)],
            pltpu.VMEM((tokens, depth), bf16),
            pltpu.VMEM((others, blocks, pieces, BLOCK, cols // pieces), bf16),
            pltpu.VMEM((others, blocks, pieces, BLOCK, cols // pieces), bf16),
            pltpu.VMEM((tokens, cols), bf16),
            pltpu.VMEM((kv_heads * blocks, 2, half, 2 * LANES), f32),
            pltpu.VMEM((kv_heads * blocks, 2, half, LANES), f32),
            pltpu.VMEM((others, BLOCK, cols), f32),
            pltpu.SemaphoreType.DMA((6,)),
            pltpu.SemaphoreType.DMA,
            pltpu.SemaphoreType.DMA((far,)),
            pltpu.SemaphoreType.DMA,
            pltpu.SemaphoreType.DMA((kv_heads + 1,)),
            pltpu.SemaphoreType.DMA,
            pltpu.SemaphoreType.DMA((others, blocks - 1 + pieces)),
            pltpu.SemaphoreType.DMA,
            pltpu.SemaphoreType.REGULAR,
        ],
        compiler_params=pltpu.CompilerParams(
            collective_id=0, has_side_effects=True, vmem_limit_bytes=51500 * 2**10
        ),
    )(
        *[
            pltpu.with_memory_space_constraint(x, pltpu.HBM)
            for x in (
                block_lists,
                doc_ids.reshape(blocks, BLOCK),
                queries,
                keys,
                values,
                w_out,
            )
        ]
    )


def solution(mesh):
    in_specs = (
        P(("dp", "seq"), "head"),
        P(("dp", "seq"), "head"),
        P(("dp", "seq"), "head"),
        P(("dp", "seq")),
        P(("dp", "seq"), None),
        P("head", None),
    )
    out_specs = P(("dp", "seq"), "head")
    return jax.shard_map(
        per_device, mesh=mesh, in_specs=in_specs, out_specs=out_specs, check_vma=False
    )
```
